512 devices in a mesh: param: 8 (over x, core), feat: 16 (over z), ex: 4 (over y).
Axes of the slice: x: 4, y: 4, z: 16, core: 2. Of those that a mesh axis runs over, the one named last changes fastest.
Arguments:
- gradients: float32 [2048, 8192], P('ex', 'param'), may hold values from -6 to 6
- projection: float32 [8192, 4, 16, 256], P('param', None, 'feat'), may hold values from -0.0625 to 0.0625
- factor: float32 [4, 16, 256, 1024], P(None, 'feat', 'param'), may hold values from -0.1875 to 0.1875
- diag_inverse: float32 [4, 256, 256], P(None, 'param'), may hold values from -1 to 1.5, as said below
- queries: float32 [4, 16, 256, 256], P(None, 'feat', 'param', 'ex'), may hold values from -6 to 6
Outputs:
- scores: float32 [256, 2048], P('param', 'ex')
- trailing: float32 [4, 16, 256, 2048], P(None, 'feat', 'param', 'ex')
- trailing_queries: float32 [4, 16, 256, 256], P(None, 'feat', 'param', 'ex')
The draws below stay inside these ranges and needn't reach their ends.
Inputs may be any that keep to these rules, and one draw needn't show every extreme that they name: `diag_inverse`: every block is upper triangular, with diagonal entries of 0.5 to 1.5.
All inputs are finite; a program needn't handle non-finite values.
Results may differ from the reference program's by a relative error of at most 0.00017.
Values sent between devices are 32-bit elements; how exact they have to be, the bound alone decides.
A program may use at most 128 MiB of HBM per device.

```python
import math
import jax
import jax.numpy as jnp
from jax import lax

PANEL = 256
SOLVED = 4
ROUNDS = 4
W = 1024
NEX = 2048
NQ = 256
P_SIZE = 8192
N_FEAT = 16


def draw_diag_inverse(key, part):
    first_key, second_key = jax.random.split(jax.random.fold_in(key, 17))
    indices = jnp.arange(PANEL)
    above = (indices[None, :] > indices[:, None]).astype(jnp.float32)
    spread = jax.random.normal(first_key, (SOLVED, PANEL, PANEL), jnp.float32)
    diagonal = jnp.exp(jax.random.uniform(second_key, (SOLVED, PANEL), jnp.float32, jnp.log(0.5), jnp.log(1.5)))
    identity = (indices[None, :] == indices[:, None]).astype(jnp.float32)
    return spread * above * (0.7 / jnp.sqrt(PANEL * 1.0)) + diagonal[:, :, None] * identity[None]


def shard_levels(own_key, shape, shards, low, largest):
    factor_of, own = 1.0, jax.random.fold_in(own_key, 6)
    for axis_at, parts in shards:
        steps = jnp.exp(jax.random.uniform(jax.random.fold_in(own, axis_at), (parts,), jnp.float32, low / len(shards), largest / len(shards)))
        factor_of = factor_of * jnp.repeat(steps, shape[axis_at] // parts).reshape([-1 if axis == axis_at else 1 for axis in range(len(shape))])
    return factor_of


def bell_draw(key, extent, width, most, cuts=(), held_as=jnp.bfloat16):
    loudness = shard_levels(key, extent, cuts, -0.22, 0.18) if cuts else 1.0
    array = jax.random.normal(key, extent, jnp.float32) * width * loudness
    return jnp.minimum(jnp.maximum(array, -most), most).astype(held_as)


def setup_inputs(seed: int = 0) -> dict:
    key_of = jax.random.split(jax.random.key(seed), 6)
    gradients = bell_draw(key_of[0], (NEX, P_SIZE), 1.0, 6.0, ((0, 4), (1, 8)), jnp.float32)
    projection = bell_draw(key_of[1], (P_SIZE, ROUNDS, N_FEAT, PANEL), P_SIZE ** -0.5, 0.0625, ((0, 8), (2, 16)), jnp.float32)
    factor = bell_draw(key_of[2], (ROUNDS, N_FEAT, PANEL, W), W ** -0.5, 0.1875, ((1, 16), (2, 8)), jnp.float32)
    diag_inverse = draw_diag_inverse(jax.random.fold_in(key_of[5], 71), 0)
    queries = bell_draw(key_of[4], (ROUNDS, N_FEAT, PANEL, NQ), 1.0, 6.0, ((1, 16), (2, 8), (3, 4)), jnp.float32)
    return dict(gradients=gradients, projection=projection, factor=factor, diag_inverse=diag_inverse, queries=queries)


exact_mode = lax.Precision.HIGHEST

def reference(gradients, projection, factor, diag_inverse, queries):
    projected = jnp.einsum('ep,pmdr->mdre', gradients, projection, precision=exact_mode)
    right_sides = jnp.concatenate([projected, queries], axis=3)
    panel_order = jnp.arange(ROUNDS)[:, None] * N_FEAT + jnp.arange(N_FEAT)[None, :]
    solved_list = []
    for panel_index in range(SOLVED):
        round_index = panel_index // N_FEAT
        owner_index = panel_index % N_FEAT
        solved = jnp.einsum('kr,kc->rc', diag_inverse[panel_index], right_sides[round_index, owner_index], precision=exact_mode)
        columns = factor[:, :, :, panel_index * PANEL:(panel_index + 1) * PANEL]
        update = jnp.einsum('mdrk,kc->mdrc', columns, solved, precision=exact_mode)
        right_sides = jnp.where((panel_order > panel_index)[:, :, None, None], right_sides - update, right_sides)
        solved_list.append(solved)
    window = jnp.concatenate(solved_list, axis=0)
    scores = jnp.einsum('kq,ke->qe', window[:, NEX:], window[:, :NEX], precision=exact_mode) / math.sqrt(W)
    return (scores, right_sides[..., :NEX], right_sides[..., NEX:])
```

```python
import math

import jax
import jax.numpy as jnp
from jax import lax
from jax.experimental import pallas as pl
from jax.experimental.pallas import tpu as pltpu
from jax.sharding import PartitionSpec as P

MESH = pl.DeviceIdType.MESH
F32 = jnp.float32
BF16 = jnp.bfloat16
CHIPS = 4
PANELS = 4
RING = 16
UP = 8
KP = 256


def halves(x):
    hi = x.astype(BF16)
    return hi, (x - hi.astype(F32)).astype(BF16)


def left3(x, axis):
    hi, lo = halves(x)
    return jnp.concatenate([hi, lo, hi], axis=axis)


def right3(x, axis):
    hi, lo = halves(x)
    return jnp.concatenate([hi, hi, lo], axis=axis)


def dot_nn(a, b):
    return jnp.dot(left3(a, 1), right3(b, 0), preferred_element_type=F32)


def dot_nt(a, b):
    return lax.dot_general(
        left3(a, 1), right3(b, 1), (((1,), (1,)), ((), ())), preferred_element_type=F32
    )


class Place:
    def __init__(self):
        self.p = lax.axis_index("param")
        self.z = lax.axis_index("feat")
        self.y = lax.axis_index("ex")
        self.x = lax.div(self.p, 2)
        self.c = lax.rem(self.p, 2)
        self.xp = lax.rem(self.x + 1, CHIPS)
        self.xm = lax.rem(self.x + CHIPS - 1, CHIPS)
        self.xo = lax.rem(self.x + 2, CHIPS)
        self.right = {"param": 2 * self.xp + self.c}
        self.left = {"param": 2 * self.xm + self.c}
        self.sib = {"param": 2 * self.x + 1 - self.c}
        self.above = {"feat": lax.rem(self.z + 1, RING)}
        self.below = {"feat": lax.rem(self.z + RING - 1, RING)}

    def slot(self, x, c):
        return 2 * x + c


def rdma(src, dst, ss, rs, dev):
    return pltpu.make_async_remote_copy(
        src_ref=src, dst_ref=dst, send_sem=ss, recv_sem=rs, device_id=dev, device_id_type=MESH
    )


class Gather:
    def __init__(self, pos, chunk, half_a, half_b, ss, rs):
        self.pos, self.chunk, self.half_a, self.half_b, self.ss, self.rs = pos, chunk, half_a, half_b, ss, rs
        q = pos
        self.own = q.slot(q.x, q.c)
        self.i_m = q.slot(q.xm, q.c)
        self.i_p = q.slot(q.xp, q.c)
        self.i_o = q.slot(q.xo, q.c)

    def copy(self, k):
        q = self.pos
        ref, dev = (
            lambda: (self.chunk(self.own), q.right),
            lambda: (self.chunk(self.own), q.left),
            lambda: (self.half_a(self.i_m), q.right),
            lambda: (self.half_b(self.i_p), q.left),
            lambda: (self.chunk(self.own), q.sib),
            lambda: (self.chunk(self.i_m), q.sib),
            lambda: (self.chunk(self.i_p), q.sib),
            lambda: (self.chunk(self.i_o), q.sib),
        )[k]()
        return rdma(ref, ref, self.ss.at[k], self.rs.at[k], dev)

    def arrive(self, ref, k):
        rdma(ref, ref, self.ss.at[k], self.rs.at[k], self.pos.sib).wait_recv()

    def start(self):
        for k in (0, 1, 4):
            self.copy(k).start()

    def mid(self):
        self.arrive(self.chunk(self.i_m), 0)
        self.copy(2).start()
        self.copy(5).start()
        self.arrive(self.chunk(self.i_p), 1)
        self.copy(3).start()
        self.copy(6).start()

    def end(self):
        self.arrive(self.half_a(self.i_o), 2)
        self.arrive(self.half_b(self.i_o), 3)
        self.copy(7).start()

    def done(self):
        q = self.pos
        for k, x in ((4, q.x), (5, q.xm), (6, q.xp), (7, q.xo)):
            self.arrive(self.chunk(q.slot(x, 1 - q.c)), k)

    def drain(self):
        for k in range(8):
            self.copy(k).wait_send()


class Reduce:
    def __init__(self, pos, parts, got, relay, direct, rows, ss, rs):
        self.pos, self.parts, self.got, self.relay, self.direct = pos, parts, got, relay, direct
        self.h, self.ss, self.rs = rows // 2, ss, rs
        self.a, self.b = pl.ds(0, self.h), pl.ds(self.h, self.h)

    def pair_copy(self, x):
        q = self.pos
        return rdma(self.parts(q.slot(x, 1 - q.c)), self.got.at[x], self.ss.at[x], self.rs.at[x], q.sib)

    def x_copy(self, k):
        q, g = self.pos, self.got
        src, dst, dev = (
            lambda: (g.at[q.xo, self.a], self.relay.at[0], q.right),
            lambda: (g.at[q.xo, self.b], self.relay.at[1], q.left),
            lambda: (g.at[q.xp, self.b], self.direct.at[0, self.b], q.right),
            lambda: (g.at[q.xm, self.a], self.direct.at[1, self.a], q.left),
            lambda: (g.at[q.xp, self.a], self.direct.at[0, self.a], q.right),
            lambda: (g.at[q.xm, self.b], self.direct.at[1, self.b], q.left),
        )[k]()
        return rdma(src, dst, self.ss.at[4 + k], self.rs.at[4 + k], dev)

    def pair(self):
        for x in range(CHIPS):
            self.pair_copy(x).start()

    def first(self):
        q, g = self.pos, self.got
        for x in range(CHIPS):
            self.pair_copy(x).wait_recv()
        for n, x in enumerate((q.xo, q.xp, q.xm, q.x)):
            g[x] = g[x] + self.parts(q.slot(x, q.c))[...]
            if n == 0:
                self.x_copy(0).start()
                self.x_copy(1).start()
            elif n < 3:
                self.x_copy(n + 1).start()

    def second(self):
        q, g = self.pos, self.got
        self.x_copy(0).wait_recv()
        g[q.xp, self.a] = g[q.xp, self.a] + self.relay[0]
        self.x_copy(4).start()
        self.x_copy(1).wait_recv()
        g[q.xm, self.b] = g[q.xm, self.b] + self.relay[1]
        self.x_copy(5).start()

    def third(self):
        for k in range(2, 6):
            self.x_copy(k).wait_recv()
        return self.got[self.pos.x] + self.direct[0] + self.direct[1]

    def drain(self):
        for x in range(CHIPS):
            self.pair_copy(x).wait_send()
        for k in range(6):
            self.x_copy(k).wait_send()


def kernel(
    g_hbm, p_hbm, f_hbm, d_hbm, q_hbm, scores_ref, trail_ref, tq_ref,
    gv, pv, g3, p3, fa, ql, yq, parts, slabs,
    pan_got, pan_relay, pan_direct, got, relay, direct,
    rbuf, db, fq0, fq1, fq2, fq3, qt, xv, av, gout, acc,
    loc, ysend, yrecv, ps, pr, ms, mr, gs, gr, zs, zr,
):
    q = Place()
    fqs = [fq0, fq1, fq2, fq3]
    own = q.slot(q.x, q.c)
    source = q.z < PANELS

    loads = [
        pltpu.make_async_copy(d_hbm, db.at[own], loc.at[0]),
        pltpu.make_async_copy(q_hbm, ql, loc.at[1]),
        pltpu.make_async_copy(g_hbm, gv, loc.at[2]),
        pltpu.make_async_copy(p_hbm, pv, loc.at[3]),
        pltpu.make_async_copy(f_hbm, fa, loc.at[4]),
    ]
    for s in loads:
        s.start()

    barrier = pltpu.get_barrier_semaphore()
    others = [{"ex": lax.rem(q.y + k, 4)} for k in (1, 2, 3)]
    for dev in [q.right, q.left, q.sib, q.above, q.below] + others:
        pl.semaphore_signal(barrier, inc=1, device_id=dev, device_id_type=MESH)
    pl.semaphore_wait(barrier, 8)

    d_gather = Gather(
        q, lambda i: db.at[i], lambda i: db.at[i, pl.ds(0, 2)], lambda i: db.at[i, pl.ds(2, 2)], gs.at[0], gr.at[0]
    )
    f_gather = [
        Gather(
            q,
            lambda i, b=fqs[s]: b.at[i],
            lambda i, b=fqs[s]: b.at[i, pl.ds(0, 16)],
            lambda i, b=fqs[s]: b.at[i, pl.ds(16, 16)],
            gs.at[1 + s],
            gr.at[1 + s],
        )
        for s in range(PANELS)
    ]
    r_gather = [
        Gather(
            q,
            lambda i, s=s: rbuf.at[s, i],
            lambda i, s=s: rbuf.at[s, i, pl.ds(0, 32)],
            lambda i, s=s: rbuf.at[s, i, pl.ds(32, 32)],
            gs.at[5 + s],
            gr.at[5 + s],
        )
        for s in range(PANELS)
    ]

    def chunk_of(kind, s):
        return fqs[s].at[own] if kind == 0 else rbuf.at[s, own]

    def hop_of(s):
        return lax.rem(q.z - s + RING, RING)

    def chain(kind, s, way):
        ref = chunk_of(kind, s)
        return rdma(ref, ref, zs.at[kind, s, way], zr.at[kind, s], (q.above, q.below)[way])

    def goes(s, way):
        hop = hop_of(s)
        return hop < UP if way == 0 else (hop == 0) | (hop > UP + 1)

    def chain_send(kind, s):
        for way in range(2):
            @pl.when(goes(s, way))
            def _(way=way):
                chain(kind, s, way).start()

    def chain_drain(kind, s):
        for way in range(2):
            @pl.when(goes(s, way))
            def _(way=way):
                chain(kind, s, way).wait_send()

    def gather_of(kind, s):
        return f_gather[s] if kind == 0 else r_gather[s]

    def send_own(kind):
        for s in range(PANELS):
            @pl.when(q.z == s)
            def _(s=s):
                chain_send(kind, s)
                gather_of(kind, s).start()

    def pass_on(kind, s):
        @pl.when(q.z != s)
        def _():
            chain(kind, s, 0).wait_recv()
            chain_send(kind, s)
            gather_of(kind, s).start()

    loads[0].wait()
    d_gather.start()

    loads[1].wait()

    def y_copy(k):
        return rdma(yq.at[q.y], yq.at[q.y], ysend.at[k], yrecv.at[k], others[k])

    for s in range(1, PANELS):
        @pl.when(q.z == s)
        def _(s=s):
            pltpu.make_async_copy(
                f_hbm.at[0, :, pl.ds(0, KP * s)], fqs[s].at[own, :, pl.ds(KP, KP * s)], loc.at[5]
            ).start()

    @pl.when(source)
    def _():
        mine = ql[0]
        both = jnp.concatenate([mine, mine], axis=1)
        lane = lax.broadcasted_iota(jnp.int32, both.shape, 1)
        yq[q.y] = jnp.where(lax.div(lane, 64) == lax.rem(q.y, 2), both, 0.0)
        for k in range(3):
            y_copy(k).start()

    loads[2].wait()
    for k in range(4):
        cols = pl.ds(k * 256, 256)
        hi, lo = halves(gv[:, cols])
        g3[:, cols] = hi
        g3[:, pl.ds(1024 + k * 256, 256)] = lo
        g3[:, pl.ds(2048 + k * 256, 256)] = hi
    loads[3].wait()

    def project(m):
        for h in range(2):
            w = pv[pl.ds(2 * m + h, 1024, stride=8), :]
            hi, lo = halves(w)
            lanes = pl.ds(128 * h, 128)
            p3[pl.ds(0, 1024), lanes] = hi
            p3[pl.ds(1024, 1024), lanes] = hi
            p3[pl.ds(2048, 1024), lanes] = lo
        for i in range(8):
            parts[m, i] = jnp.dot(g3[pl.ds(64 * i, 64), :], p3[...], preferred_element_type=F32)

    panel = Reduce(q, lambda i: parts.at[0, i], pan_got, pan_relay, pan_direct, 64, ps, pr)
    main = Reduce(q, lambda i: slabs.at[i], got, relay, direct, 512, ms, mr)

    project(0)
    pl.when(source)(panel.pair)

    @pl.when(source)
    def _():
        for k in range(3):
            y_copy(k).wait_recv()
        for s in range(PANELS):
            @pl.when(q.z == s)
            def _(s=s):
                fqs[s][own, :, pl.ds(0, 128)] = yq[0] + yq[1]
                fqs[s][own, :, pl.ds(128, 128)] = yq[2] + yq[3]
                if s > 0:
                    pltpu.make_async_copy(
                        f_hbm.at[0, :, pl.ds(0, KP * s)], fqs[s].at[own, :, pl.ds(KP, KP * s)], loc.at[5]
                    ).wait()

    project(1)
    pl.when(source)(panel.first)
    send_own(0)
    project(2)
    pl.when(source)(panel.second)
    d_gather.mid()
    project(3)

    @pl.when(source)
    def _():
        rbuf[q.z, own] = panel.third()
    send_own(1)

    lane = lax.broadcasted_iota(jnp.int32, (512, 128), 1)
    for h in range(2):
        cols = pl.ds(128 * h, 128)
        rounds = [parts[m, :, :, cols].reshape(512, 128) for m in range(4)]
        for k in range(4):
            slab = None
            for m in range(4):
                turn = (32 * (m - k)) % 128
                moved = pltpu.roll(rounds[m], turn, 1) if turn else rounds[m]
                slab = moved if slab is None else jnp.where(lax.div(lane, 32) == m, moved, slab)
            slabs[4 * h + k] = slab
    main.pair()
    d_gather.end()

    order = (3, 2, 1, 0)
    pass_on(0, 3)
    main.first()
    pass_on(0, 2)
    f_gather[3].mid()
    pass_on(0, 1)
    f_gather[2].mid()
    f_gather[3].end()
    main.second()
    pass_on(0, 0)
    f_gather[1].mid()
    f_gather[2].end()
    pass_on(1, 3)
    f_gather[0].mid()
    f_gather[1].end()
    pass_on(1, 2)
    f_gather[0].end()
    r_gather[3].mid()
    pass_on(1, 1)
    r_gather[2].mid()
    r_gather[3].end()
    pass_on(1, 0)
    r_gather[1].mid()
    r_gather[2].end()
    r_gather[0].mid()
    r_gather[1].end()
    r_gather[0].end()

    d_gather.done()
    for s in order:
        f_gather[s].done()
    loads[4].wait()

    def inverse(j):
        return db[:, j].reshape(KP, KP)

    def block(l, j):
        return fqs[l][:, :, pl.ds(KP * (j + 1), KP)].reshape(KP, KP)

    for s in range(PANELS):
        qt[:, pl.ds(KP * s, KP)] = jnp.transpose(fqs[s][:, :, pl.ds(0, KP)].reshape(KP, KP))
    mine = pl.ds(pl.multiple_of(32 * own, 32), 32)
    for j in range(PANELS):
        y = qt[mine, pl.ds(KP * j, KP)]
        for l in range(j):
            y = y - dot_nt(xv[:, pl.ds(KP * l, KP)], block(j, l))
        xv[:, pl.ds(KP * j, KP)] = dot_nn(y, inverse(j))
    for j in range(PANELS):
        cols = pl.ds(KP * j, KP)
        f = fa[:, :, cols]
        m_of = lax.broadcasted_iota(jnp.int32, f.shape, 0)
        f = jnp.where(m_of * RING + q.z > j, f, 0.0)
        av[pl.ds(0, 128), cols] = f.reshape(128, KP)
        av[pl.ds(128, 32), cols] = xv[:, cols]
    for j in reversed(range(PANELS)):
        cols = pl.ds(KP * j, KP)
        y = av[:, cols]
        for l in range(j + 1, PANELS):
            y = y - dot_nn(gout[:, pl.ds(KP * l, KP)], block(l, j))
        gout[:, cols] = dot_nt(y, inverse(j))

    tq = jnp.zeros((128, 64), F32)
    yrows = pl.ds(pl.multiple_of(64 * q.y, 64), 64)
    for s in range(PANELS):
        cols = pl.ds(KP * s, KP)
        tq = tq + dot_nt(gout[pl.ds(0, 128), cols], qt[yrows, cols])
    tq_ref[...] = ql[...].reshape(128, 64) - tq

    for n, s in enumerate(order):
        r_gather[s].done()
        part = dot_nt(gout[:, pl.ds(KP * s, KP)], rbuf[s].reshape(512, KP))
        acc[...] = part if n == 0 else acc[...] + part
    slab = main.third()
    trail_ref[...] = jnp.transpose(slab) - acc[pl.ds(0, 128), :]
    scores_ref[...] = acc[pl.ds(128, 32), :] * (1.0 / math.sqrt(KP * PANELS))

    for kind in range(2):
        for s in range(PANELS):
            chain_drain(kind, s)
            gather_of(kind, s).drain()
    d_gather.drain()
    main.drain()

    @pl.when(source)
    def _():
        panel.drain()
        for k in range(3):
            y_copy(k).wait_send()


def per_device(gradients, projection, factor, diag_inverse, queries):
    vm = lambda *shape: pltpu.VMEM(shape, F32)
    dma = pltpu.SemaphoreType.DMA
    any_space = pl.BlockSpec(memory_space=pl.ANY)
    vmem_space = pl.BlockSpec(memory_space=pltpu.VMEM)
    scores, trailing, trailing_queries = pl.pallas_call(
        kernel,
        out_shape=(
            jax.ShapeDtypeStruct((32, 512), F32),
            jax.ShapeDtypeStruct((128, 512), F32),
            jax.ShapeDtypeStruct((128, 64), F32),
        ),
        in_specs=[any_space] * 5,
        out_specs=(vmem_space,) * 3,
        scratch_shapes=[
            vm(512, 1024), vm(8192, 128),
            pltpu.VMEM((512, 3072), BF16), pltpu.VMEM((3072, 256), BF16),
            vm(4, 32, 1024), vm(4, 32, 64), vm(4, 32, 128),
            vm(4, 8, 64, 256), vm(8, 512, 128),
            vm(4, 64, 256), vm(2, 32, 256), vm(2, 64, 256),
            vm(4, 512, 128), vm(2, 256, 128), vm(2, 512, 128),
            vm(4, 8, 64, 256), vm(8, 4, 32, 256),
            vm(8, 32, 256), vm(8, 32, 512), vm(8, 32, 768), vm(8, 32, 1024),
            vm(256, 1024), vm(32, 1024), vm(160, 1024), vm(160, 1024), vm(160, 512),
            dma((6,)), dma((3,)), dma((3,)),
            dma((10,)), dma((10,)), dma((10,)), dma((10,)),
            dma((9, 8)), dma((9, 8)), dma((2, 4, 2)), dma((2, 4)),
        ],
        compiler_params=pltpu.CompilerParams(
            collective_id=0, has_side_effects=True, vmem_limit_bytes=60 * 1024 * 1024
        ),
    )(
        gradients,
        projection.reshape(8192, 128),
        factor.reshape(4, 32, 1024),
        diag_inverse,
        queries.reshape(4, 32, 64),
    )
    return (
        scores,
        trailing.reshape(4, 1, 32, 512),
        trailing_queries.reshape(4, 1, 32, 64),
    )


def solution(mesh):
    return jax.shard_map(
        per_device,
        mesh=mesh,
        in_specs=(
            P("ex", "param"),
            P("param", None, "feat", None),
            P(None, "feat", "param", None),
            P(None, "param", None),
            P(None, "feat", "param", "ex"),
        ),
        out_specs=(
            P("param", "ex"),
            P(None, "feat", "param", "ex"),
            P(None, "feat", "param", "ex"),
        ),
        check_vma=False,
    )
```

```python
import math

import jax
import jax.numpy as jnp
from jax import lax
from jax.experimental import pallas as pl
from jax.experimental.pallas import tpu as pltpu
from jax.sharding import PartitionSpec as P

MESH = pl.DeviceIdType.MESH
F32 = jnp.float32
BF16 = jnp.bfloat16
CHIPS = 4
PANELS = 4
RING = 16
UP = 8
KP = 256


def halves(x):
    hi = x.astype(BF16)
    return hi, (x - hi.astype(F32)).astype(BF16)


def left3(x, axis):
    hi, lo = halves(x)
    return jnp.concatenate([hi, lo, hi], axis=axis)


def right3(x, axis):
    hi, lo = halves(x)
    return jnp.concatenate([hi, hi, lo], axis=axis)


def dot_nn(a, b):
    return jnp.dot(left3(a, 1), right3(b, 0), preferred_element_type=F32)


def dot_nt(a, b):
    return lax.dot_general(
        left3(a, 1), right3(b, 1), (((1,), (1,)), ((), ())), preferred_element_type=F32
    )


class Place:
    def __init__(self):
        self.p = lax.axis_index("param")
        self.z = lax.axis_index("feat")
        self.y = lax.axis_index("ex")
        self.x = lax.div(self.p, 2)
        self.c = lax.rem(self.p, 2)
        self.xp = lax.rem(self.x + 1, CHIPS)
        self.xm = lax.rem(self.x + CHIPS - 1, CHIPS)
        self.xo = lax.rem(self.x + 2, CHIPS)
        self.right = {"param": 2 * self.xp + self.c}
        self.left = {"param": 2 * self.xm + self.c}
        self.sib = {"param": 2 * self.x + 1 - self.c}
        self.front = {"ex": lax.rem(self.y + 1, 4)}
        self.back = {"ex": lax.rem(self.y + 3, 4)}
        self.above = {"feat": lax.rem(self.z + 1, RING)}
        self.below = {"feat": lax.rem(self.z + RING - 1, RING)}

    def slot(self, x, c):
        return 2 * x + c


def rdma(src, dst, ss, rs, dev):
    return pltpu.make_async_remote_copy(
        src_ref=src, dst_ref=dst, send_sem=ss, recv_sem=rs, device_id=dev, device_id_type=MESH
    )


class Ring:
    def __init__(self, me, ahead, behind, sib, chunk, half_a, half_b, other, ss, rs):
        self.me, self.m, self.p, self.o = me, lax.rem(me + 3, 4), lax.rem(me + 1, 4), lax.rem(me + 2, 4)
        self.ahead, self.behind, self.sib = ahead, behind, sib
        self.chunk, self.half_a, self.half_b, self.other = chunk, half_a, half_b, other
        self.ss, self.rs = ss, rs

    def copy(self, k):
        ref, dev = (
            lambda: (self.chunk(self.me), self.ahead),
            lambda: (self.chunk(self.me), self.behind),
            lambda: (self.half_a(self.m), self.ahead),
            lambda: (self.half_b(self.p), self.behind),
            lambda: (self.chunk(self.me), self.sib),
            lambda: (self.chunk(self.m), self.sib),
            lambda: (self.chunk(self.p), self.sib),
            lambda: (self.chunk(self.o), self.sib),
        )[k]()
        return rdma(ref, ref, self.ss.at[k], self.rs.at[k], dev)

    def send(self, k):
        if k < 4 or self.other is not None:
            self.copy(k).start()

    def arrive(self, ref, k):
        rdma(ref, ref, self.ss.at[k], self.rs.at[k], self.sib).wait_recv()

    def start(self):
        for k in (0, 1, 4):
            self.send(k)

    def mid(self):
        self.arrive(self.chunk(self.m), 0)
        self.send(2)
        self.send(5)
        self.arrive(self.chunk(self.p), 1)
        self.send(3)
        self.send(6)

    def end(self):
        self.arrive(self.half_a(self.o), 2)
        self.arrive(self.half_b(self.o), 3)
        self.send(7)

    def done(self):
        for k, n in ((4, self.me), (5, self.m), (6, self.p), (7, self.o)):
            self.arrive(self.other(n), k)

    def drain(self):
        for k in range(4 if self.other is None else 8):
            self.copy(k).wait_send()


class Reduce:
    def __init__(self, pos, parts, got, relay, direct, rows, ss, rs):
        self.pos, self.parts, self.got, self.relay, self.direct = pos, parts, got, relay, direct
        self.h, self.ss, self.rs = rows // 2, ss, rs
        self.a, self.b = pl.ds(0, self.h), pl.ds(self.h, self.h)

    def pair_copy(self, x):
        q = self.pos
        return rdma(self.parts(q.slot(x, 1 - q.c)), self.got.at[x], self.ss.at[x], self.rs.at[x], q.sib)

    def x_copy(self, k):
        q, g = self.pos, self.got
        src, dst, dev = (
            lambda: (g.at[q.xo, self.a], self.relay.at[0], q.right),
            lambda: (g.at[q.xo, self.b], self.relay.at[1], q.left),
            lambda: (g.at[q.xp, self.b], self.direct.at[0, self.b], q.right),
            lambda: (g.at[q.xm, self.a], self.direct.at[1, self.a], q.left),
            lambda: (g.at[q.xp, self.a], self.direct.at[0, self.a], q.right),
            lambda: (g.at[q.xm, self.b], self.direct.at[1, self.b], q.left),
        )[k]()
        return rdma(src, dst, self.ss.at[4 + k], self.rs.at[4 + k], dev)

    def pair(self):
        for x in range(CHIPS):
            self.pair_copy(x).start()

    def first(self):
        q, g = self.pos, self.got
        for x in range(CHIPS):
            self.pair_copy(x).wait_recv()
        for n, x in enumerate((q.xo, q.xp, q.xm, q.x)):
            g[x] = g[x] + self.parts(q.slot(x, q.c))[...]
            if n == 0:
                self.x_copy(0).start()
                self.x_copy(1).start()
            elif n < 3:
                self.x_copy(n + 1).start()

    def second(self):
        q, g = self.pos, self.got
        self.x_copy(0).wait_recv()
        g[q.xp, self.a] = g[q.xp, self.a] + self.relay[0]
        self.x_copy(4).start()
        self.x_copy(1).wait_recv()
        g[q.xm, self.b] = g[q.xm, self.b] + self.relay[1]
        self.x_copy(5).start()

    def third(self):
        for k in range(2, 6):
            self.x_copy(k).wait_recv()
        return self.got[self.pos.x] + self.direct[0] + self.direct[1]

    def drain(self):
        for x in range(CHIPS):
            self.pair_copy(x).wait_send()
        for k in range(6):
            self.x_copy(k).wait_send()


def kernel(
    g_hbm, p_hbm, f_hbm, d_hbm, q_hbm, scores_ref, trail_ref, tq_ref,
    gv, pv, g3, p3, fa, ql, parts, slabs,
    pan_got, pan_relay, pan_direct, got, relay, direct,
    rbuf, db, fq, qs, qt, xv, av, gout, acc,
    loc, ps, pr, ms, mr, gs, gr, zs, zr, fs, fr,
):
    q = Place()
    own = q.slot(q.x, q.c)
    source = q.z < PANELS

    def lanes_of(s):
        return 128 * s * (s + 1), KP * (s + 1)

    def load(k):
        return (
            lambda: pltpu.make_async_copy(g_hbm, gv, loc.at[0]),
            lambda: pltpu.make_async_copy(p_hbm, pv, loc.at[1]),
            lambda: pltpu.make_async_copy(d_hbm.at[q.y], db.at[q.c, q.x, q.y], loc.at[2]),
            lambda: pltpu.make_async_copy(q_hbm, ql, loc.at[3]),
            lambda: pltpu.make_async_copy(f_hbm, fa, loc.at[4]),
        )[k]()

    for k in range(5):
        load(k).start()

    def rows_of(s):
        at, wide = lanes_of(s)
        return pltpu.make_async_copy(
            f_hbm.at[0, pl.ds(pl.multiple_of(8 * q.y, 8), 8), pl.ds(0, KP * s)],
            fq.at[q.c, q.x, q.y, :, pl.ds(at + KP, KP * s)],
            loc.at[5],
        )

    for s in range(1, PANELS):
        @pl.when(q.z == s)
        def _(s=s):
            rows_of(s).start()

    barrier = pltpu.get_barrier_semaphore()

    def greet(dev):
        pl.semaphore_signal(barrier, inc=1, device_id=dev, device_id_type=MESH)

    for dev in [q.right, q.left, q.sib, q.front, q.back, q.above, q.below]:
        greet(dev)
    for s in range(PANELS):
        hop = lax.rem(q.z - s + RING, RING)

        @pl.when((hop > 1) & (hop < RING - 1))
        def _(s=s):
            greet({"feat": s})

    low, high = pl.ds(0, 2), pl.ds(2, 2)
    r_ring = [
        Ring(
            q.x, q.right, q.left, q.sib,
            lambda n, s=s: rbuf.at[s, q.slot(n, q.c)],
            lambda n, s=s: rbuf.at[s, q.slot(n, q.c), pl.ds(0, 32)],
            lambda n, s=s: rbuf.at[s, q.slot(n, q.c), pl.ds(32, 32)],
            lambda n, s=s: rbuf.at[s, q.slot(n, 1 - q.c)],
            gs.at[s], gr.at[s],
        )
        for s in range(PANELS)
    ]
    fx = Ring(
        q.x, q.right, q.left, q.sib,
        lambda n: fq.at[q.c, n, q.y],
        lambda n: fq.at[q.c, n, q.y, :, pl.ds(0, 1280)],
        lambda n: fq.at[q.c, n, q.y, :, pl.ds(1280, 1280)],
        None, gs.at[4], gr.at[4],
    )
    fy = Ring(
        q.y, q.front, q.back, q.sib,
        lambda n: fq.at[q.c, :, n],
        lambda n: fq.at[q.c, low, n],
        lambda n: fq.at[q.c, high, n],
        lambda n: fq.at[1 - q.c, :, n],
        gs.at[5], gr.at[5],
    )
    dx = Ring(
        q.x, q.right, q.left, q.sib,
        lambda n: db.at[q.c, n, q.y],
        lambda n: db.at[q.c, n, q.y, pl.ds(0, 16)],
        lambda n: db.at[q.c, n, q.y, pl.ds(16, 16)],
        None, gs.at[6], gr.at[6],
    )
    dy = Ring(
        q.y, q.front, q.back, q.sib,
        lambda n: db.at[q.c, :, n],
        lambda n: db.at[q.c, low, n],
        lambda n: db.at[q.c, high, n],
        lambda n: db.at[1 - q.c, :, n],
        gs.at[7], gr.at[7],
    )

    def hop_of(s):
        return lax.rem(q.z - s + RING, RING)

    def chain(s, k, way):
        ref = rbuf.at[s, own, pl.ds(16 * k, 16)]
        return rdma(ref, ref, zs.at[s, k, way], zr.at[s, k], (q.above, q.below)[way])

    def goes(s, way):
        hop = hop_of(s)
        return hop < UP if way == 0 else (hop == 0) | (hop > UP + 1)

    def chain_send(s, k):
        for way in range(2):
            @pl.when(goes(s, way))
            def _(way=way):
                chain(s, k, way).start()

    def pass_on(s):
        @pl.when(q.z != s)
        def _():
            for k in range(4):
                chain(s, k, 0).wait_recv()
                chain_send(s, k)
            r_ring[s].start()

    def row_copy(s, k):
        at, wide = lanes_of(s)
        ref = fq.at[q.c, q.x, q.y, :, pl.ds(at, wide)]
        return rdma(ref, ref, fs.at[k], fr.at[s], {"feat": lax.rem(q.z + k, RING)})

    def rows_arrive():
        for s in range(PANELS):
            @pl.when(q.z != s)
            def _(s=s):
                row_copy(s, 1).wait_recv()

    load(0).wait()
    for k in range(4):
        cols = pl.ds(k * 256, 256)
        hi, lo = halves(gv[:, cols])
        g3[:, cols] = hi
        g3[:, pl.ds(1024 + k * 256, 256)] = lo
        g3[:, pl.ds(2048 + k * 256, 256)] = hi
    load(1).wait()

    def project(m):
        for h in range(2):
            w = pv[pl.ds(2 * m + h, 1024, stride=8), :]
            hi, lo = halves(w)
            lanes = pl.ds(128 * h, 128)
            p3[pl.ds(0, 1024), lanes] = hi
            p3[pl.ds(1024, 1024), lanes] = hi
            p3[pl.ds(2048, 1024), lanes] = lo
        for i in range(8):
            parts[m, i] = jnp.dot(g3[pl.ds(64 * i, 64), :], p3[...], preferred_element_type=F32)

    panel = Reduce(q, lambda i: parts.at[0, i], pan_got, pan_relay, pan_direct, 64, ps, pr)
    main = Reduce(q, lambda i: slabs.at[i], got, relay, direct, 512, ms, mr)

    load(3).wait()
    for s in range(PANELS):
        @pl.when(q.z == s)
        def _(s=s):
            at, wide = lanes_of(s)
            mine = ql[0]
            fq[q.c, q.x, q.y, :, pl.ds(at, KP)] = jnp.concatenate(
                [mine[8 * k : 8 * k + 8] for k in range(4)], axis=1
            )
            if s > 0:
                rows_of(s).wait()

    project(0)
    pl.semaphore_wait(barrier, jnp.where(source, 5 + RING - 1, 7))
    pl.when(source)(panel.pair)
    load(2).wait()
    dx.start()
    for s in range(PANELS):
        @pl.when(q.z == s)
        def _(s=s):
            for k in (1, 15, 2, 14, 3, 13, 4, 12, 5, 11, 6, 10, 7, 9, 8):
                row_copy(s, k).start()

    project(1)
    pl.when(source)(panel.first)
    dx.mid()
    project(2)
    pl.when(source)(panel.second)
    dx.end()
    dy.start()

    near = (q.z <= PANELS) | (q.z == RING - 1)
    far = (q.z > PANELS + 2) & (q.z < RING - 3)
    between = jnp.logical_not(near | far)

    @pl.when(near)
    def _():
        rows_arrive()
        fx.start()

    project(3)

    @pl.when(source)
    def _():
        rbuf[q.z, own] = panel.third()
        for s in range(PANELS):
            @pl.when(q.z == s)
            def _(s=s):
                for k in range(4):
                    chain_send(s, k)
                r_ring[s].start()

    dy.mid()
    pl.when(near)(fx.mid)

    lane = lax.broadcasted_iota(jnp.int32, (512, 128), 1)
    for h in range(2):
        cols = pl.ds(128 * h, 128)
        rounds = [parts[m, :, :, cols].reshape(512, 128) for m in range(4)]
        for k in range(4):
            slab = None
            for m in range(4):
                turn = (32 * (m - k)) % 128
                moved = pltpu.roll(rounds[m], turn, 1) if turn else rounds[m]
                slab = moved if slab is None else jnp.where(lax.div(lane, 32) == m, moved, slab)
            slabs[4 * h + k] = slab
    main.pair()
    dy.end()

    def panels_pass():
        pass_on(3)
        pass_on(2)
        r_ring[3].mid()
        pass_on(1)
        r_ring[2].mid()
        r_ring[3].end()
        pass_on(0)
        r_ring[1].mid()
        r_ring[2].end()

    @pl.when(near)
    def _():
        fx.end()
        fy.start()
        panels_pass()
        main.first()
        fy.mid()
        main.second()

    @pl.when(between)
    def _():
        rows_arrive()
        fx.start()
        main.first()
        fx.mid()
        fx.end()
        fy.start()
        panels_pass()
        main.second()
        fy.mid()

    @pl.when(far)
    def _():
        main.first()
        rows_arrive()
        fx.start()
        main.second()
        fx.mid()
        fx.end()
        fy.start()
        panels_pass()
        fy.mid()

    r_ring[0].mid()
    r_ring[1].end()
    fy.end()
    r_ring[0].end()

    dy.done()
    fy.done()
    load(4).wait()
    places = [(i % 2, i // 2) for i in range(8)]

    def inverse(j):
        return jnp.concatenate([db[c, x, j] for c, x in places], axis=0)

    def block(l, j):
        cols = pl.ds(lanes_of(l)[0] + KP * (j + 1), KP)
        return jnp.concatenate([fq[c, x, :, :, cols].reshape(32, KP) for c, x in places], axis=0)

    for s in range(PANELS):
        cols = pl.ds(lanes_of(s)[0], KP)
        held = [fq[:, :, y, :, cols].reshape(64, KP) for y in range(4)]
        for k in range(4):
            rows = jnp.concatenate([held[y][:, 64 * k : 64 * k + 64] for y in range(4)], axis=1)
            for c in range(2):
                for x in range(CHIPS):
                    n = 8 * (4 * c + x)
                    qs[2 * x + c, k] = rows[n : n + 8]
        qt[:, pl.ds(KP * s, KP)] = jnp.transpose(qs[...].reshape(KP, KP))
    mine = pl.ds(pl.multiple_of(32 * own, 32), 32)
    for j in range(PANELS):
        y = qt[mine, pl.ds(KP * j, KP)]
        for l in range(j):
            y = y - dot_nt(xv[:, pl.ds(KP * l, KP)], block(j, l))
        xv[:, pl.ds(KP * j, KP)] = dot_nn(y, inverse(j))
    for j in range(PANELS):
        cols = pl.ds(KP * j, KP)
        f = fa[:, :, cols]
        m_of = lax.broadcasted_iota(jnp.int32, f.shape, 0)
        f = jnp.where(m_of * RING + q.z > j, f, 0.0)
        av[pl.ds(0, 128), cols] = f.reshape(128, KP)
        av[pl.ds(128, 32), cols] = xv[:, cols]
    for j in reversed(range(PANELS)):
        cols = pl.ds(KP * j, KP)
        y = av[:, cols]
        for l in range(j + 1, PANELS):
            y = y - dot_nn(gout[:, pl.ds(KP * l, KP)], block(l, j))
        gout[:, cols] = dot_nt(y, inverse(j))

    tq = jnp.zeros((128, 64), F32)
    yrows = pl.ds(pl.multiple_of(64 * q.y, 64), 64)
    for s in range(PANELS):
        cols = pl.ds(KP * s, KP)
        tq = tq + dot_nt(gout[pl.ds(0, 128), cols], qt[yrows, cols])
    tq_ref[...] = ql[...].reshape(128, 64) - tq

    for n, s in enumerate((3, 2, 1, 0)):
        r_ring[s].done()
        part = dot_nt(gout[:, pl.ds(KP * s, KP)], rbuf[s].reshape(512, KP))
        acc[...] = part if n == 0 else acc[...] + part
    slab = main.third()
    trail_ref[...] = jnp.transpose(slab) - acc[pl.ds(0, 128), :]
    scores_ref[...] = acc[pl.ds(128, 32), :] * (1.0 / math.sqrt(KP * PANELS))

    for s in range(PANELS):
        for k in range(4):
            for way in range(2):
                @pl.when(goes(s, way))
                def _(s=s, k=k, way=way):
                    chain(s, k, way).wait_send()
        r_ring[s].drain()

        @pl.when(q.z == s)
        def _(s=s):
            for k in range(1, RING):
                row_copy(s, k).wait_send()
    for ring in (fx, fy, dx, dy):
        ring.drain()
    main.drain()
    pl.when(source)(panel.drain)


def finish(scores_in, trail_in, tq_in, scores_ref, trail_ref, tq_ref):
    scores_ref[...] = scores_in[...]
    trail_ref[...] = trail_in[...]
    tq_ref[...] = tq_in[...]


def per_device(gradients, projection, factor, diag_inverse, queries):
    vm = lambda *shape: pltpu.VMEM(shape, F32)
    dma = pltpu.SemaphoreType.DMA
    any_space = pl.BlockSpec(memory_space=pl.ANY)
    vmem_space = pl.BlockSpec(memory_space=pltpu.VMEM)
    shapes = (
        jax.ShapeDtypeStruct((32, 512), F32),
        jax.ShapeDtypeStruct((128, 512), F32),
        jax.ShapeDtypeStruct((128, 64), F32),
    )
    results = pl.pallas_call(
        kernel,
        out_shape=shapes,
        in_specs=[any_space] * 5,
        out_specs=(vmem_space,) * 3,
        scratch_shapes=[
            vm(512, 1024), vm(8192, 128),
            pltpu.VMEM((512, 3072), BF16), pltpu.VMEM((3072, 256), BF16),
            vm(4, 32, 1024), vm(4, 32, 64),
            vm(4, 8, 64, 256), vm(8, 512, 128),
            vm(4, 64, 256), vm(2, 32, 256), vm(2, 64, 256),
            vm(4, 512, 128), vm(2, 256, 128), vm(2, 512, 128),
            vm(4, 8, 64, 256), vm(2, 4, 4, 32, 256), vm(2, 4, 4, 8, 2560),
            vm(8, 4, 8, 256), vm(256, 1024), vm(32, 1024), vm(160, 1024), vm(160, 1024), vm(160, 512),
            dma((6,)), dma((10,)), dma((10,)), dma((10,)), dma((10,)),
            dma((8, 8)), dma((8, 8)), dma((4, 4, 2)), dma((4, 4)), dma((16,)), dma((4,)),
        ],
        compiler_params=pltpu.CompilerParams(
            collective_id=0, has_side_effects=True, vmem_limit_bytes=60 * 1024 * 1024
        ),
    )(
        gradients,
        projection.reshape(8192, 128),
        factor.reshape(4, 32, 1024),
        diag_inverse,
        queries.reshape(4, 32, 64),
    )
    scores, trailing, trailing_queries = pl.pallas_call(
        finish, out_shape=shapes, in_specs=[vmem_space] * 3, out_specs=(vmem_space,) * 3
    )(*results)
    return (
        scores,
        trailing.reshape(4, 1, 32, 512),
        trailing_queries.reshape(4, 1, 32, 64),
    )


def solution(mesh):
    return jax.shard_map(
        per_device,
        mesh=mesh,
        in_specs=(
            P("ex", "param"),
            P("param", None, "feat", None),
            P(None, "feat", "param", None),
            P(None, "param", None),
            P(None, "feat", "param", "ex"),
        ),
        out_specs=(
            P("param", "ex"),
            P(None, "feat", "param", "ex"),
            P(None, "feat", "param", "ex"),
        ),
        check_vma=False,
    )
```

```python
import math

import jax
import jax.numpy as jnp
from jax import lax
from jax.experimental import pallas as pl
from jax.experimental.pallas import tpu as pltpu
from jax.sharding import PartitionSpec as P

MESH = pl.DeviceIdType.MESH
F32 = jnp.float32
BF16 = jnp.bfloat16
CHIPS = 4
PANELS = 4
RING = 16
UP = 8
KP = 256


def halves(x):
    hi = x.astype(BF16)
    return hi, (x - hi.astype(F32)).astype(BF16)


def left3(x, axis):
    hi, lo = halves(x)
    return jnp.concatenate([hi, lo, hi], axis=axis)


def right3(x, axis):
    hi, lo = halves(x)
    return jnp.concatenate([hi, hi, lo], axis=axis)


def dot_nn(a, b):
    return jnp.dot(left3(a, 1), right3(b, 0), preferred_element_type=F32)


def dot_nt(a, b):
    return lax.dot_general(
        left3(a, 1), right3(b, 1), (((1,), (1,)), ((), ())), preferred_element_type=F32
    )


class Place:
    def __init__(self):
        self.p = lax.axis_index("param")
        self.z = lax.axis_index("feat")
        self.y = lax.axis_index("ex")
        self.x = lax.div(self.p, 2)
        self.c = lax.rem(self.p, 2)
        self.xp = lax.rem(self.x + 1, CHIPS)
        self.xm = lax.rem(self.x + CHIPS - 1, CHIPS)
        self.xo = lax.rem(self.x + 2, CHIPS)
        self.right = {"param": 2 * self.xp + self.c}
        self.left = {"param": 2 * self.xm + self.c}
        self.sib = {"param": 2 * self.x + 1 - self.c}
        self.front = {"ex": lax.rem(self.y + 1, 4)}
        self.back = {"ex": lax.rem(self.y + 3, 4)}
        self.above = {"feat": lax.rem(self.z + 1, RING)}
        self.below = {"feat": lax.rem(self.z + RING - 1, RING)}

    def slot(self, x, c):
        return 2 * x + c


def rdma(src, dst, ss, rs, dev):
    return pltpu.make_async_remote_copy(
        src_ref=src, dst_ref=dst, send_sem=ss, recv_sem=rs, device_id=dev, device_id_type=MESH
    )


class Ring:
    def __init__(self, me, ahead, behind, sib, chunk, half_a, half_b, other, ss, rs):
        self.me, self.m, self.p, self.o = me, lax.rem(me + 3, 4), lax.rem(me + 1, 4), lax.rem(me + 2, 4)
        self.ahead, self.behind, self.sib = ahead, behind, sib
        self.chunk, self.half_a, self.half_b, self.other = chunk, half_a, half_b, other
        self.ss, self.rs = ss, rs

    def copy(self, k):
        ref, dev = (
            lambda: (self.chunk(self.me), self.ahead),
            lambda: (self.chunk(self.me), self.behind),
            lambda: (self.half_a(self.m), self.ahead),
            lambda: (self.half_b(self.p), self.behind),
            lambda: (self.chunk(self.me), self.sib),
            lambda: (self.chunk(self.m), self.sib),
            lambda: (self.chunk(self.p), self.sib),
            lambda: (self.chunk(self.o), self.sib),
        )[k]()
        return rdma(ref, ref, self.ss.at[k], self.rs.at[k], dev)

    def send(self, k):
        if k < 4 or self.other is not None:
            self.copy(k).start()

    def arrive(self, ref, k):
        rdma(ref, ref, self.ss.at[k], self.rs.at[k], self.sib).wait_recv()

    def start(self):
        for k in (0, 1, 4):
            self.send(k)

    def mid(self):
        self.arrive(self.chunk(self.m), 0)
        self.send(2)
        self.send(5)
        self.arrive(self.chunk(self.p), 1)
        self.send(3)
        self.send(6)

    def end(self):
        self.arrive(self.half_a(self.o), 2)
        self.arrive(self.half_b(self.o), 3)
        self.send(7)

    def done(self):
        for k, n in ((4, self.me), (5, self.m), (6, self.p), (7, self.o)):
            self.arrive(self.other(n), k)

    def drain(self):
        for k in range(4 if self.other is None else 8):
            self.copy(k).wait_send()


class Both:
    def __init__(self, *rings):
        self.rings = rings

    def __getattr__(self, name):
        def step():
            for ring in self.rings:
                getattr(ring, name)()

        return step


class Reduce:
    def __init__(self, pos, parts, got, relay, direct, rows, ss, rs):
        self.pos, self.parts, self.got, self.relay, self.direct = pos, parts, got, relay, direct
        self.h, self.ss, self.rs = rows // 2, ss, rs
        self.a, self.b = pl.ds(0, self.h), pl.ds(self.h, self.h)

    def pair_copy(self, x):
        q = self.pos
        return rdma(self.parts(q.slot(x, 1 - q.c)), self.got.at[x], self.ss.at[x], self.rs.at[x], q.sib)

    def x_copy(self, k):
        q, g = self.pos, self.got
        src, dst, dev = (
            lambda: (g.at[q.xo, self.a], self.relay.at[0], q.right),
            lambda: (g.at[q.xo, self.b], self.relay.at[1], q.left),
            lambda: (g.at[q.xp, self.b], self.direct.at[0, self.b], q.right),
            lambda: (g.at[q.xm, self.a], self.direct.at[1, self.a], q.left),
            lambda: (g.at[q.xp, self.a], self.direct.at[0, self.a], q.right),
            lambda: (g.at[q.xm, self.b], self.direct.at[1, self.b], q.left),
        )[k]()
        return rdma(src, dst, self.ss.at[4 + k], self.rs.at[4 + k], dev)

    def pair(self):
        for x in range(CHIPS):
            self.pair_copy(x).start()

    def first(self):
        q, g = self.pos, self.got
        for x in range(CHIPS):
            self.pair_copy(x).wait_recv()
        for n, x in enumerate((q.xo, q.xp, q.xm, q.x)):
            g[x] = g[x] + self.parts(q.slot(x, q.c))[...]
            if n == 0:
                self.x_copy(0).start()
                self.x_copy(1).start()
            elif n < 3:
                self.x_copy(n + 1).start()

    def second(self):
        q, g = self.pos, self.got
        self.x_copy(0).wait_recv()
        g[q.xp, self.a] = g[q.xp, self.a] + self.relay[0]
        self.x_copy(4).start()
        self.x_copy(1).wait_recv()
        g[q.xm, self.b] = g[q.xm, self.b] + self.relay[1]
        self.x_copy(5).start()

    def third(self):
        for k in range(2, 6):
            self.x_copy(k).wait_recv()
        return self.got[self.pos.x] + self.direct[0] + self.direct[1]

    def drain(self):
        for x in range(CHIPS):
            self.pair_copy(x).wait_send()
        for k in range(6):
            self.x_copy(k).wait_send()


def kernel(
    g_hbm, p_hbm, f_hbm, d_hbm, q_hbm, scores_ref, trail_ref, tq_ref,
    gv, pv, g3, p3, fa, ql, parts, slabs,
    pan_got, pan_relay, pan_direct, got, relay, direct,
    rbuf, db, fb, qb, qs, qt, xv, av, gout, acc,
    dn, dt, loc, ps, pr, ms, mr, gs, gr, zs, zr, fs, fr,
):
    q = Place()
    own = q.slot(q.x, q.c)
    source = q.z < PANELS

    def lane_of(s):
        return 128 * s * (s - 1)

    def load(k):
        return (
            lambda: pltpu.make_async_copy(g_hbm, gv, loc.at[0]),
            lambda: pltpu.make_async_copy(p_hbm, pv, loc.at[1]),
            lambda: pltpu.make_async_copy(d_hbm.at[q.y], db.at[q.c, q.x, q.y], loc.at[2]),
            lambda: pltpu.make_async_copy(q_hbm, ql, loc.at[3]),
            lambda: pltpu.make_async_copy(f_hbm, fa, loc.at[4]),
        )[k]()

    for k in range(5):
        load(k).start()

    def rows_of(s):
        return pltpu.make_async_copy(
            f_hbm.at[0, pl.ds(pl.multiple_of(8 * q.y, 8), 8), pl.ds(0, KP * s)],
            fb.at[q.c, q.x, q.y, :, pl.ds(lane_of(s), KP * s)],
            loc.at[5],
        )

    for s in range(1, PANELS):
        @pl.when(q.z == s)
        def _(s=s):
            rows_of(s).start()

    barrier = pltpu.get_barrier_semaphore()

    def greet(dev):
        pl.semaphore_signal(barrier, inc=1, device_id=dev, device_id_type=MESH)

    for dev in [q.right, q.left, q.sib, q.front, q.back, q.above, q.below]:
        greet(dev)
    low, high = pl.ds(0, 2), pl.ds(2, 2)
    r_ring = [
        Ring(
            q.x, q.right, q.left, q.sib,
            lambda n, s=s: rbuf.at[s, q.slot(n, q.c)],
            lambda n, s=s: rbuf.at[s, q.slot(n, q.c), pl.ds(0, 32)],
            lambda n, s=s: rbuf.at[s, q.slot(n, q.c), pl.ds(32, 32)],
            lambda n, s=s: rbuf.at[s, q.slot(n, 1 - q.c)],
            gs.at[s], gr.at[s],
        )
        for s in range(PANELS)
    ]
    fx = Both(
        Ring(
            q.x, q.right, q.left, q.sib,
            lambda n: fb.at[q.c, n, q.y],
            lambda n: fb.at[q.c, n, q.y, :, pl.ds(0, 768)],
            lambda n: fb.at[q.c, n, q.y, :, pl.ds(768, 768)],
            None, gs.at[4], gr.at[4],
        ),
        Ring(
            q.y, q.front, q.back, q.sib,
            lambda n: qb.at[q.c, q.x, n],
            lambda n: qb.at[q.c, q.x, n, :, pl.ds(0, 512)],
            lambda n: qb.at[q.c, q.x, n, :, pl.ds(512, 512)],
            None, gs.at[8], gr.at[8],
        ),
    )
    fy = Both(
        Ring(
            q.y, q.front, q.back, q.sib,
            lambda n: fb.at[q.c, :, n],
            lambda n: fb.at[q.c, low, n],
            lambda n: fb.at[q.c, high, n],
            lambda n: fb.at[1 - q.c, :, n],
            gs.at[5], gr.at[5],
        ),
        Ring(
            q.x, q.right, q.left, q.sib,
            lambda n: qb.at[q.c, n],
            lambda n: qb.at[q.c, n, low],
            lambda n: qb.at[q.c, n, high],
            lambda n: qb.at[1 - q.c, n],
            gs.at[9], gr.at[9],
        ),
    )
    dx = Ring(
        q.x, q.right, q.left, q.sib,
        lambda n: db.at[q.c, n, q.y],
        lambda n: db.at[q.c, n, q.y, pl.ds(0, 16)],
        lambda n: db.at[q.c, n, q.y, pl.ds(16, 16)],
        None, gs.at[6], gr.at[6],
    )
    dy = Ring(
        q.y, q.front, q.back, q.sib,
        lambda n: db.at[q.c, :, n],
        lambda n: db.at[q.c, low, n],
        lambda n: db.at[q.c, high, n],
        lambda n: db.at[1 - q.c, :, n],
        gs.at[7], gr.at[7],
    )

    def hop_of(s):
        return lax.rem(q.z - s + RING, RING)

    def chain(s, k, way):
        ref = rbuf.at[s, own, pl.ds(16 * k, 16)]
        return rdma(ref, ref, zs.at[s, k, way], zr.at[s, k], (q.above, q.below)[way])

    def goes(s, way):
        hop = hop_of(s)
        return hop < UP if way == 0 else (hop == 0) | (hop > UP + 1)

    def chain_send(s, k):
        for way in range(2):
            @pl.when(goes(s, way))
            def _(way=way):
                chain(s, k, way).start()

    def pass_on(s):
        @pl.when(q.z != s)
        def _():
            for k in range(4):
                chain(s, k, 0).wait_recv()
                chain_send(s, k)

    def row_copy(s, way, part):
        if part == 0:
            ref = qb.at[q.c, q.x, q.y, :, pl.ds(KP * s, KP)]
        else:
            ref = fb.at[q.c, q.x, q.y, :, pl.ds(lane_of(s), KP * s)]
        return rdma(ref, ref, fs.at[s, way, part], fr.at[s, part], (q.above, q.below)[way])

    def parts_of(s):
        return range(1 if s == 0 else 2)

    def row_send(s):
        for way in range(2):
            @pl.when(goes(s, way))
            def _(way=way):
                for part in parts_of(s):
                    row_copy(s, way, part).start()

    def rows_hop(t):
        for s in range(PANELS):
            @pl.when((hop_of(s) == t) | ((hop_of(s) == RING - t) & (t < UP)))
            def _(s=s):
                for part in parts_of(s):
                    row_copy(s, 0, part).wait_recv()
                row_send(s)

    load(0).wait()
    for k in range(4):
        cols = pl.ds(k * 256, 256)
        hi, lo = halves(gv[:, cols])
        g3[:, cols] = hi
        g3[:, pl.ds(1024 + k * 256, 256)] = lo
        g3[:, pl.ds(2048 + k * 256, 256)] = hi
    load(3).wait()
    for s in range(PANELS):
        @pl.when(q.z == s)
        def _(s=s):
            mine = ql[0]
            qb[q.c, q.x, q.y, :, pl.ds(KP * s, KP)] = jnp.concatenate(
                [mine[8 * k : 8 * k + 8] for k in range(4)], axis=1
            )
            if s > 0:
                rows_of(s).wait()
    load(2).wait()
    pl.semaphore_wait(barrier, 7)
    for s in range(PANELS):
        @pl.when(q.z == s)
        def _(s=s):
            row_send(s)
    dx.start()
    load(1).wait()

    def project(m):
        for h in range(2):
            w = pv[pl.ds(2 * m + h, 1024, stride=8), :]
            hi, lo = halves(w)
            lanes = pl.ds(128 * h, 128)
            p3[pl.ds(0, 1024), lanes] = hi
            p3[pl.ds(1024, 1024), lanes] = hi
            p3[pl.ds(2048, 1024), lanes] = lo
        parts[m] = jnp.dot(g3[...], p3[...], preferred_element_type=F32).reshape(8, 64, 256)

    panel = Reduce(q, lambda i: parts.at[0, i], pan_got, pan_relay, pan_direct, 64, ps, pr)
    main = Reduce(q, lambda i: slabs.at[i], got, relay, direct, 512, ms, mr)

    down, upward = (0, 1, 2, 3), (3, 2, 1, 0)
    climbs = (q.z > 1) & (q.z < UP + 2)

    def sides(which):
        return (which & climbs, upward), (which & jnp.logical_not(climbs), down)

    def panels_over_x():
        for s in upward:
            r_ring[s].start()

    project(0)
    pl.when(source)(panel.pair)
    project(1)
    pl.when(source)(panel.first)

    @pl.when(jnp.logical_not(source))
    def _():
        rows_hop(1)

    project(2)

    @pl.when(source)
    def _():
        rows_hop(1)
        panel.second()
        rows_hop(2)

    @pl.when(jnp.logical_not(source))
    def _():
        rows_hop(2)
        dx.mid()

    project(3)

    @pl.when(source)
    def _():
        rbuf[q.z, own] = panel.third()
        for s in range(PANELS):
            @pl.when(q.z == s)
            def _(s=s):
                for k in range(4):
                    chain_send(s, k)
        dx.mid()

    rows_hop(3)

    for side, order in sides(source):
        @pl.when(side)
        def _(order=order):
            fx.start()
            pass_on(order[0])
            pass_on(order[1])
            dx.end()
            dy.start()
            pass_on(order[2])
            pass_on(order[3])
            fx.mid()

    lane = lax.broadcasted_iota(jnp.int32, (512, 128), 1)
    for h in range(2):
        cols = pl.ds(128 * h, 128)
        rounds = [parts[m, :, :, cols].reshape(512, 128) for m in range(4)]
        for k in range(4):
            slab = None
            for m in range(4):
                turn = (32 * (m - k)) % 128
                moved = pltpu.roll(rounds[m], turn, 1) if turn else rounds[m]
                slab = moved if slab is None else jnp.where(lax.div(lane, 32) == m, moved, slab)
            slabs[4 * h + k] = slab
    main.pair()
    rows_hop(4)

    @pl.when(jnp.logical_not(source))
    def _():
        dx.end()
        dy.start()

    near = (q.z == PANELS) | (q.z == RING - 1)
    between = ((q.z > PANELS) & (q.z < PANELS + 3)) | ((q.z > RING - 4) & (q.z < RING - 1))
    late = (q.z == PANELS + 3) | (q.z == RING - 4)
    far = (q.z > PANELS + 3) & (q.z < RING - 4)

    @pl.when(source)
    def _():
        fx.end()
        fy.start()
        main.first()
        panels_over_x()
        dy.mid()
        main.second()
        dy.end()

    for side, order in sides(near):
        @pl.when(side)
        def _(order=order):
            fx.start()
            pass_on(order[0])
            pass_on(order[1])
            fx.mid()
            main.first()
            pass_on(order[2])
            fx.end()
            fy.start()
            pass_on(order[3])
            dy.mid()
            panels_over_x()
            main.second()
            dy.end()

    for side, order in sides(between):
        @pl.when(side)
        def _(order=order):
            main.first()
            rows_hop(5)
            rows_hop(6)
            fx.start()
            pass_on(order[0])
            pass_on(order[1])
            fx.mid()
            pass_on(order[2])
            fx.end()
            fy.start()
            pass_on(order[3])
            main.second()
            panels_over_x()
            dy.mid()
            dy.end()

    for side, order in sides(late):
        @pl.when(side)
        def _(order=order):
            main.first()
            rows_hop(5)
            dy.mid()
            rows_hop(6)
            rows_hop(7)
            fx.start()
            pass_on(order[0])
            pass_on(order[1])
            main.second()
            fx.mid()
            pass_on(order[2])
            fx.end()
            fy.start()
            pass_on(order[3])
            panels_over_x()
            dy.end()

    for side, order in sides(far):
        @pl.when(side)
        def _(order=order):
            main.first()
            rows_hop(5)
            dy.mid()
            rows_hop(6)
            dy.end()
            main.second()
            rows_hop(7)
            pass_on(order[0])
            rows_hop(8)
            fx.start()
            pass_on(order[1])
            fx.mid()
            pass_on(order[2])
            fx.end()
            fy.start()
            pass_on(order[3])
            panels_over_x()

    for s in (3, 2, 1, 0):
        r_ring[s].mid()
    fy.mid()
    for s in (3, 2, 1, 0):
        r_ring[s].end()
    dy.done()
    load(4).wait()
    places = [(i % 2, i // 2) for i in range(8)]
    for j in range(PANELS):
        inverse = jnp.concatenate([db[c, x, j] for c, x in places], axis=0)
        dn[j] = right3(inverse, 0)
        dt[j] = right3(inverse, 1)
    fy.end()

    fy.done()

    def block(l, j):
        cols = pl.ds(lane_of(l) + KP * j, KP)
        return jnp.concatenate([fb[c, x, :, :, cols].reshape(32, KP) for c, x in places], axis=0)

    for s in range(PANELS):
        cols = pl.ds(KP * s, KP)
        held = [qb[:, :, y, :, cols].reshape(64, KP) for y in range(4)]
        for k in range(4):
            rows = jnp.concatenate([held[y][:, 64 * k : 64 * k + 64] for y in range(4)], axis=1)
            for c in range(2):
                for x in range(CHIPS):
                    n = 8 * (4 * c + x)
                    qs[2 * x + c, k] = rows[n : n + 8]
        qt[:, pl.ds(KP * s, KP)] = jnp.transpose(qs[...].reshape(KP, KP))
    mine = pl.ds(pl.multiple_of(32 * own, 32), 32)
    for j in range(PANELS):
        y = qt[mine, pl.ds(KP * j, KP)]
        for l in range(j):
            y = y - dot_nt(xv[:, pl.ds(KP * l, KP)], block(j, l))
        xv[:, pl.ds(KP * j, KP)] = jnp.dot(left3(y, 1), dn[j], preferred_element_type=F32)
    for j in range(PANELS):
        cols = pl.ds(KP * j, KP)
        f = fa[:, :, cols]
        m_of = lax.broadcasted_iota(jnp.int32, f.shape, 0)
        f = jnp.where(m_of * RING + q.z > j, f, 0.0)
        av[pl.ds(0, 128), cols] = f.reshape(128, KP)
        av[pl.ds(128, 32), cols] = xv[:, cols]
    for j in reversed(range(PANELS)):
        cols = pl.ds(KP * j, KP)
        y = av[:, cols]
        for l in range(j + 1, PANELS):
            y = y - dot_nn(gout[:, pl.ds(KP * l, KP)], block(l, j))
        gout[:, cols] = lax.dot_general(
            left3(y, 1), dt[j], (((1,), (1,)), ((), ())), preferred_element_type=F32
        )

    tq = jnp.zeros((128, 64), F32)
    yrows = pl.ds(pl.multiple_of(64 * q.y, 64), 64)
    for s in range(PANELS):
        cols = pl.ds(KP * s, KP)
        tq = tq + dot_nt(gout[pl.ds(0, 128), cols], qt[yrows, cols])
    tq_ref[...] = ql[...].reshape(128, 64) - tq

    for n, s in enumerate((3, 2, 1, 0)):
        r_ring[s].done()
        part = dot_nt(gout[:, pl.ds(KP * s, KP)], rbuf[s].reshape(512, KP))
        acc[...] = part if n == 0 else acc[...] + part
    slab = main.third()
    trail_ref[...] = jnp.transpose(slab) - acc[pl.ds(0, 128), :]
    scores_ref[...] = acc[pl.ds(128, 32), :] * (1.0 / math.sqrt(KP * PANELS))

    for s in range(PANELS):
        for k in range(4):
            for way in range(2):
                @pl.when(goes(s, way))
                def _(s=s, k=k, way=way):
                    chain(s, k, way).wait_send()
        r_ring[s].drain()

        for way in range(2):
            @pl.when(goes(s, way))
            def _(s=s, way=way):
                for part in parts_of(s):
                    row_copy(s, way, part).wait_send()
    for ring in (fx, fy, dx, dy):
        ring.drain()
    main.drain()
    pl.when(source)(panel.drain)


def finish(scores_in, trail_in, tq_in, scores_ref, trail_ref, tq_ref):
    scores_ref[...] = scores_in[...]
    trail_ref[...] = trail_in[...]
    tq_ref[...] = tq_in[...]


def per_device(gradients, projection, factor, diag_inverse, queries):
    vm = lambda *shape: pltpu.VMEM(shape, F32)
    dma = pltpu.SemaphoreType.DMA
    any_space = pl.BlockSpec(memory_space=pl.ANY)
    vmem_space = pl.BlockSpec(memory_space=pltpu.VMEM)
    shapes = (
        jax.ShapeDtypeStruct((32, 512), F32),
        jax.ShapeDtypeStruct((128, 512), F32),
        jax.ShapeDtypeStruct((128, 64), F32),
    )
    results = pl.pallas_call(
        kernel,
        out_shape=shapes,
        in_specs=[any_space] * 5,
        out_specs=(vmem_space,) * 3,
        scratch_shapes=[
            vm(512, 1024), vm(8192, 128),
            pltpu.VMEM((512, 3072), BF16), pltpu.VMEM((3072, 256), BF16),
            vm(4, 32, 1024), vm(4, 32, 64),
            vm(4, 8, 64, 256), vm(8, 512, 128),
            vm(4, 64, 256), vm(2, 32, 256), vm(2, 64, 256),
            vm(4, 512, 128), vm(2, 256, 128), vm(2, 512, 128),
            vm(4, 8, 64, 256), vm(2, 4, 4, 32, 256), vm(2, 4, 4, 8, 1536), vm(2, 4, 4, 8, 1024),
            vm(8, 4, 8, 256), vm(256, 1024), vm(32, 1024), vm(160, 1024), vm(160, 1024), vm(160, 512),
            pltpu.VMEM((4, 768, 256), BF16), pltpu.VMEM((4, 256, 768), BF16),
            dma((6,)), dma((10,)), dma((10,)), dma((10,)), dma((10,)),
            dma((10, 8)), dma((10, 8)), dma((4, 4, 2)), dma((4, 4)), dma((4, 2, 2)), dma((4, 2)),
        ],
        compiler_params=pltpu.CompilerParams(
            collective_id=0, has_side_effects=True, vmem_limit_bytes=60 * 1024 * 1024
        ),
    )(
        gradients,
        projection.reshape(8192, 128),
        factor.reshape(4, 32, 1024),
        diag_inverse,
        queries.reshape(4, 32, 64),
    )
    scores, trailing, trailing_queries = pl.pallas_call(
        finish, out_shape=shapes, in_specs=[vmem_space] * 3, out_specs=(vmem_space,) * 3
    )(*results)
    return (
        scores,
        trailing.reshape(4, 1, 32, 512),
        trailing_queries.reshape(4, 1, 32, 64),
    )


def solution(mesh):
    return jax.shard_map(
        per_device,
        mesh=mesh,
        in_specs=(
            P("ex", "param"),
            P("param", None, "feat", None),
            P(None, "feat", "param", None),
            P(None, "param", None),
            P(None, "feat", "param", "ex"),
        ),
        out_specs=(
            P("param", "ex"),
            P(None, "feat", "param", "ex"),
            P(None, "feat", "param", "ex"),
        ),
        check_vma=False,
    )
```

```python
import math

import jax
import jax.numpy as jnp
from jax import lax
from jax.experimental import pallas as pl
from jax.experimental.pallas import tpu as pltpu
from jax.sharding import PartitionSpec as P

MESH = pl.DeviceIdType.MESH
F32 = jnp.float32
BF16 = jnp.bfloat16
CHIPS = 4
PANELS = 4
RING = 16
UP = 8
KP = 256


def halves(x):
    hi = x.astype(BF16)
    return hi, (x - hi.astype(F32)).astype(BF16)


def left3(x, axis):
    hi, lo = halves(x)
    return jnp.concatenate([hi, lo, hi], axis=axis)


def right3(x, axis):
    hi, lo = halves(x)
    return jnp.concatenate([hi, hi, lo], axis=axis)


def dot_nn(a, b):
    return jnp.dot(left3(a, 1), right3(b, 0), preferred_element_type=F32)


def dot_nt(a, b):
    return lax.dot_general(
        left3(a, 1), right3(b, 1), (((1,), (1,)), ((), ())), preferred_element_type=F32
    )


class Place:
    def __init__(self):
        self.p = lax.axis_index("param")
        self.z = lax.axis_index("feat")
        self.y = lax.axis_index("ex")
        self.x = lax.div(self.p, 2)
        self.c = lax.rem(self.p, 2)
        self.xp = lax.rem(self.x + 1, CHIPS)
        self.xm = lax.rem(self.x + CHIPS - 1, CHIPS)
        self.xo = lax.rem(self.x + 2, CHIPS)
        self.right = {"param": 2 * self.xp + self.c}
        self.left = {"param": 2 * self.xm + self.c}
        self.sib = {"param": 2 * self.x + 1 - self.c}
        self.front = {"ex": lax.rem(self.y + 1, 4)}
        self.back = {"ex": lax.rem(self.y + 3, 4)}
        self.above = {"feat": lax.rem(self.z + 1, RING)}
        self.below = {"feat": lax.rem(self.z + RING - 1, RING)}

    def slot(self, x, c):
        return 2 * x + c


def rdma(src, dst, ss, rs, dev):
    return pltpu.make_async_remote_copy(
        src_ref=src, dst_ref=dst, send_sem=ss, recv_sem=rs, device_id=dev, device_id_type=MESH
    )


class Ring:
    def __init__(self, me, ahead, behind, sib, chunk, half_a, half_b, other, ss, rs):
        self.me, self.m, self.p, self.o = me, lax.rem(me + 3, 4), lax.rem(me + 1, 4), lax.rem(me + 2, 4)
        self.ahead, self.behind, self.sib = ahead, behind, sib
        self.chunk, self.half_a, self.half_b, self.other = chunk, half_a, half_b, other
        self.ss, self.rs = ss, rs

    def copy(self, k):
        ref, dev = (
            lambda: (self.chunk(self.me), self.ahead),
            lambda: (self.chunk(self.me), self.behind),
            lambda: (self.half_a(self.m), self.ahead),
            lambda: (self.half_b(self.p), self.behind),
            lambda: (self.chunk(self.me), self.sib),
            lambda: (self.chunk(self.m), self.sib),
            lambda: (self.chunk(self.p), self.sib),
            lambda: (self.chunk(self.o), self.sib),
        )[k]()
        return rdma(ref, ref, self.ss.at[k], self.rs.at[k], dev)

    def send(self, k):
        if k < 4 or self.other is not None:
            self.copy(k).start()

    def arrive(self, ref, k):
        rdma(ref, ref, self.ss.at[k], self.rs.at[k], self.sib).wait_recv()

    def start(self):
        for k in (0, 1, 4):
            self.send(k)

    def mid(self):
        self.arrive(self.chunk(self.m), 0)
        self.send(2)
        self.send(5)
        self.arrive(self.chunk(self.p), 1)
        self.send(3)
        self.send(6)

    def end(self):
        self.arrive(self.half_a(self.o), 2)
        self.arrive(self.half_b(self.o), 3)
        self.send(7)

    def done(self):
        for k, n in ((4, self.me), (5, self.m), (6, self.p), (7, self.o)):
            self.arrive(self.other(n), k)

    def drain(self):
        for k in range(4 if self.other is None else 8):
            self.copy(k).wait_send()


class Both:
    def __init__(self, *rings):
        self.rings = rings

    def __getattr__(self, name):
        def step():
            for ring in self.rings:
                getattr(ring, name)()

        return step


class Reduce:
    def __init__(self, pos, parts, got, relay, direct, rows, ss, rs):
        self.pos, self.parts, self.got, self.relay, self.direct = pos, parts, got, relay, direct
        self.h, self.ss, self.rs = rows // 2, ss, rs
        self.a, self.b = pl.ds(0, self.h), pl.ds(self.h, self.h)

    def pair_copy(self, x):
        q = self.pos
        return rdma(self.parts(q.slot(x, 1 - q.c)), self.got.at[x], self.ss.at[x], self.rs.at[x], q.sib)

    def x_copy(self, k):
        q, g = self.pos, self.got
        src, dst, dev = (
            lambda: (g.at[q.xo, self.a], self.relay.at[0], q.right),
            lambda: (g.at[q.xo, self.b], self.relay.at[1], q.left),
            lambda: (g.at[q.xp, self.b], self.direct.at[0, self.b], q.right),
            lambda: (g.at[q.xm, self.a], self.direct.at[1, self.a], q.left),
            lambda: (g.at[q.xp, self.a], self.direct.at[0, self.a], q.right),
            lambda: (g.at[q.xm, self.b], self.direct.at[1, self.b], q.left),
        )[k]()
        return rdma(src, dst, self.ss.at[4 + k], self.rs.at[4 + k], dev)

    def pair(self):
        for x in range(CHIPS):
            self.pair_copy(x).start()

    def first(self):
        q, g = self.pos, self.got
        for x in range(CHIPS):
            self.pair_copy(x).wait_recv()
        for n, x in enumerate((q.xo, q.xp, q.xm, q.x)):
            g[x] = g[x] + self.parts(q.slot(x, q.c))[...]
            if n == 0:
                self.x_copy(0).start()
                self.x_copy(1).start()
            elif n < 3:
                self.x_copy(n + 1).start()

    def second(self):
        q, g = self.pos, self.got
        self.x_copy(0).wait_recv()
        g[q.xp, self.a] = g[q.xp, self.a] + self.relay[0]
        self.x_copy(4).start()
        self.x_copy(1).wait_recv()
        g[q.xm, self.b] = g[q.xm, self.b] + self.relay[1]
        self.x_copy(5).start()

    def third(self):
        for k in range(2, 6):
            self.x_copy(k).wait_recv()
        return self.got[self.pos.x] + self.direct[0] + self.direct[1]

    def drain(self):
        for x in range(CHIPS):
            self.pair_copy(x).wait_send()
        for k in range(6):
            self.x_copy(k).wait_send()


def kernel(
    g_hbm, p_hbm, f_hbm, d_hbm, q_hbm, scores_ref, trail_ref, tq_ref,
    gv, pv, g3, p3, fa, ql, parts, slabs,
    pan_got, pan_relay, pan_direct, got, relay, direct,
    rbuf, db, fb, qb, qs, qt, xv, av, gout, acc,
    dn, dt, loc, ps, pr, ms, mr, gs, gr, zs, zr, fs, fr,
):
    q = Place()
    own = q.slot(q.x, q.c)
    source = q.z < PANELS

    def lane_of(s):
        return 128 * s * (s - 1)

    def load(k):
        return (
            lambda: pltpu.make_async_copy(g_hbm, gv, loc.at[0]),
            lambda: pltpu.make_async_copy(p_hbm, pv, loc.at[1]),
            lambda: pltpu.make_async_copy(d_hbm.at[q.y], db.at[q.c, q.x, q.y], loc.at[2]),
            lambda: pltpu.make_async_copy(q_hbm, ql, loc.at[3]),
            lambda: pltpu.make_async_copy(f_hbm, fa, loc.at[4]),
        )[k]()

    for k in range(5):
        load(k).start()

    def rows_of(s):
        return pltpu.make_async_copy(
            f_hbm.at[0, pl.ds(pl.multiple_of(8 * q.y, 8), 8), pl.ds(0, KP * s)],
            fb.at[q.c, q.x, q.y, :, pl.ds(lane_of(s), KP * s)],
            loc.at[5],
        )

    for s in range(1, PANELS):
        @pl.when(q.z == s)
        def _(s=s):
            rows_of(s).start()

    barrier = pltpu.get_barrier_semaphore()

    def greet(dev):
        pl.semaphore_signal(barrier, inc=1, device_id=dev, device_id_type=MESH)

    for dev in [q.right, q.left, q.sib, q.front, q.back, q.above, q.below]:
        greet(dev)
    low, high = pl.ds(0, 2), pl.ds(2, 2)
    r_ring = [
        Ring(
            q.x, q.right, q.left, q.sib,
            lambda n, s=s: rbuf.at[s, q.slot(n, q.c)],
            lambda n, s=s: rbuf.at[s, q.slot(n, q.c), pl.ds(0, 32)],
            lambda n, s=s: rbuf.at[s, q.slot(n, q.c), pl.ds(32, 32)],
            lambda n, s=s: rbuf.at[s, q.slot(n, 1 - q.c)],
            gs.at[s], gr.at[s],
        )
        for s in range(PANELS)
    ]
    fx = Both(
        Ring(
            q.x, q.right, q.left, q.sib,
            lambda n: fb.at[q.c, n, q.y],
            lambda n: fb.at[q.c, n, q.y, :, pl.ds(0, 768)],
            lambda n: fb.at[q.c, n, q.y, :, pl.ds(768, 768)],
            None, gs.at[4], gr.at[4],
        ),
        Ring(
            q.y, q.front, q.back, q.sib,
            lambda n: qb.at[q.c, q.x, n],
            lambda n: qb.at[q.c, q.x, n, :, pl.ds(0, 512)],
            lambda n: qb.at[q.c, q.x, n, :, pl.ds(512, 512)],
            None, gs.at[8], gr.at[8],
        ),
    )
    fy = Both(
        Ring(
            q.y, q.front, q.back, q.sib,
            lambda n: fb.at[q.c, :, n],
            lambda n: fb.at[q.c, low, n],
            lambda n: fb.at[q.c, high, n],
            lambda n: fb.at[1 - q.c, :, n],
            gs.at[5], gr.at[5],
        ),
        Ring(
            q.x, q.right, q.left, q.sib,
            lambda n: qb.at[q.c, n],
            lambda n: qb.at[q.c, n, low],
            lambda n: qb.at[q.c, n, high],
            lambda n: qb.at[1 - q.c, n],
            gs.at[9], gr.at[9],
        ),
    )
    dx = Ring(
        q.x, q.right, q.left, q.sib,
        lambda n: db.at[q.c, n, q.y],
        lambda n: db.at[q.c, n, q.y, pl.ds(0, 16)],
        lambda n: db.at[q.c, n, q.y, pl.ds(16, 16)],
        None, gs.at[6], gr.at[6],
    )
    dy = Ring(
        q.y, q.front, q.back, q.sib,
        lambda n: db.at[q.c, :, n],
        lambda n: db.at[q.c, low, n],
        lambda n: db.at[q.c, high, n],
        lambda n: db.at[1 - q.c, :, n],
        gs.at[7], gr.at[7],
    )

    def hop_of(s):
        return lax.rem(q.z - s + RING, RING)

    def chain(s, k, way):
        ref = rbuf.at[s, own, pl.ds(16 * k, 16)]
        return rdma(ref, ref, zs.at[s, k, way], zr.at[s, k], (q.above, q.below)[way])

    def goes(s, way):
        hop = hop_of(s)
        return hop < UP if way == 0 else (hop == 0) | (hop > UP + 1)

    def chain_send(s, k):
        for way in range(2):
            @pl.when(goes(s, way))
            def _(way=way):
                chain(s, k, way).start()

    def pass_on(s):
        @pl.when(q.z != s)
        def _():
            for k in range(4):
                chain(s, k, 0).wait_recv()
                chain_send(s, k)

    def row_copy(s, way, part):
        if part == 0:
            ref = qb.at[q.c, q.x, q.y, :, pl.ds(KP * s, KP)]
        else:
            ref = fb.at[q.c, q.x, q.y, :, pl.ds(lane_of(s), KP * s)]
        return rdma(ref, ref, fs.at[s, way, part], fr.at[s, part], (q.above, q.below)[way])

    def parts_of(s):
        return range(1 if s == 0 else 2)

    def row_send(s):
        for way in range(2):
            @pl.when(goes(s, way))
            def _(way=way):
                for part in parts_of(s):
                    row_copy(s, way, part).start()

    def rows_hop(t):
        for s in range(PANELS):
            @pl.when((hop_of(s) == t) | ((hop_of(s) == RING - t) & (t < UP)))
            def _(s=s):
                for part in parts_of(s):
                    row_copy(s, 0, part).wait_recv()
                row_send(s)

    load(0).wait()
    for k in range(4):
        cols = pl.ds(k * 256, 256)
        hi, lo = halves(gv[:, cols])
        g3[:, cols] = hi
        g3[:, pl.ds(1024 + k * 256, 256)] = lo
        g3[:, pl.ds(2048 + k * 256, 256)] = hi
    load(3).wait()
    for s in range(PANELS):
        @pl.when(q.z == s)
        def _(s=s):
            mine = ql[0]
            qb[q.c, q.x, q.y, :, pl.ds(KP * s, KP)] = jnp.concatenate(
                [mine[8 * k : 8 * k + 8] for k in range(4)], axis=1
            )
            if s > 0:
                rows_of(s).wait()
    load(2).wait()
    pl.semaphore_wait(barrier, 7)
    for s in range(PANELS):
        @pl.when(q.z == s)
        def _(s=s):
            row_send(s)
    dx.start()
    load(1).wait()

    def project(m):
        for h in range(2):
            w = pv[pl.ds(2 * m + h, 1024, stride=8), :]
            hi, lo = halves(w)
            lanes = pl.ds(128 * h, 128)
            p3[pl.ds(0, 1024), lanes] = hi
            p3[pl.ds(1024, 1024), lanes] = hi
            p3[pl.ds(2048, 1024), lanes] = lo
        parts[m] = jnp.dot(g3[...], p3[...], preferred_element_type=F32).reshape(8, 64, 256)

    panel = Reduce(q, lambda i: parts.at[0, i], pan_got, pan_relay, pan_direct, 64, ps, pr)
    main = Reduce(q, lambda i: slabs.at[i], got, relay, direct, 512, ms, mr)

    down, upward = (0, 1, 2, 3), (3, 2, 1, 0)
    climbs = (q.z > 1) & (q.z < UP + 2)

    def sides(which):
        return (which & climbs, upward), (which & jnp.logical_not(climbs), down)

    project(0)
    pl.when(source)(panel.pair)
    project(1)
    pl.when(source)(panel.first)

    @pl.when(jnp.logical_not(source))
    def _():
        rows_hop(1)

    project(2)

    @pl.when(source)
    def _():
        rows_hop(1)
        panel.second()
        rows_hop(2)

    @pl.when(jnp.logical_not(source))
    def _():
        rows_hop(2)
        dx.mid()

    project(3)

    @pl.when(source)
    def _():
        rbuf[q.z, own] = panel.third()
        for s in range(PANELS):
            @pl.when(q.z == s)
            def _(s=s):
                for k in range(4):
                    chain_send(s, k)
        dx.mid()

    rows_hop(3)

    lane = lax.broadcasted_iota(jnp.int32, (512, 128), 1)
    for h in range(2):
        cols = pl.ds(128 * h, 128)
        rounds = [parts[m, :, :, cols].reshape(512, 128) for m in range(4)]
        for k in range(4):
            slab = None
            for m in range(4):
                turn = (32 * (m - k)) % 128
                moved = pltpu.roll(rounds[m], turn, 1) if turn else rounds[m]
                slab = moved if slab is None else jnp.where(lax.div(lane, 32) == m, moved, slab)
            slabs[4 * h + k] = slab
    main.pair()

    @pl.when(jnp.logical_not(source))
    def _():
        rows_hop(4)
        dx.end()
        dy.start()

    near = (q.z == PANELS) | (q.z == RING - 1)
    between = ((q.z > PANELS) & (q.z < PANELS + 3)) | ((q.z > RING - 4) & (q.z < RING - 1))
    late = (q.z == PANELS + 3) | (q.z == RING - 4)
    far = (q.z > PANELS + 3) & (q.z < RING - 4)

    def over_x(s):
        r_ring[s].start()

    for side, order in sides(source):
        @pl.when(side)
        def _(order=order):
            rows_hop(4)
            fx.start()
            pass_on(order[0])
            pass_on(order[1])
            main.first()
            dx.end()
            dy.start()
            pass_on(order[2])
            fx.mid()
            pass_on(order[3])
            fx.end()
            fy.start()
            for s in order:
                over_x(s)
            main.second()
            dy.mid()
            dy.end()

    for side, order in sides(near):
        @pl.when(side)
        def _(order=order):
            fx.start()
            pass_on(order[0])
            main.first()
            pass_on(order[1])
            fx.mid()
            pass_on(order[2])
            fx.end()
            fy.start()
            for s in order[:3]:
                over_x(s)
            pass_on(order[3])
            over_x(order[3])
            main.second()
            dy.mid()
            dy.end()

    for side, order in sides(between):
        @pl.when(side)
        def _(order=order):
            main.first()
            rows_hop(5)
            rows_hop(6)
            fx.start()
            pass_on(order[0])
            main.second()
            fx.mid()
            pass_on(order[1])
            fx.end()
            fy.start()
            for s in order[:2]:
                over_x(s)
            pass_on(order[2])
            over_x(order[2])
            pass_on(order[3])
            over_x(order[3])
            dy.mid()
            dy.end()

    for side, order in sides(late):
        @pl.when(side)
        def _(order=order):
            main.first()
            rows_hop(5)
            dy.mid()
            rows_hop(6)
            main.second()
            rows_hop(7)
            fx.start()
            pass_on(order[0])
            fx.mid()
            pass_on(order[1])
            fx.end()
            fy.start()
            for s in order[:2]:
                over_x(s)
            pass_on(order[2])
            over_x(order[2])
            pass_on(order[3])
            over_x(order[3])
            dy.end()

    for side, order in sides(far):
        @pl.when(side)
        def _(order=order):
            main.first()
            rows_hop(5)
            dy.mid()
            rows_hop(6)
            dy.end()
            main.second()
            rows_hop(7)
            rows_hop(8)
            fx.start()
            if order is down:
                fx.mid()
            pass_on(order[0])
            if order is down:
                fx.end()
                fy.start()
            else:
                fx.mid()
            pass_on(order[1])
            if order is upward:
                fx.end()
                fy.start()
            for s in order[:2]:
                over_x(s)
            pass_on(order[2])
            over_x(order[2])
            pass_on(order[3])
            over_x(order[3])

    for side, order in sides(q.z >= 0):
        @pl.when(side)
        def _(order=order):
            for s in order:
                r_ring[s].mid()
            fy.mid()

    dy.done()
    load(4).wait()
    places = [(i % 2, i // 2) for i in range(8)]
    for j in range(PANELS):
        inverse = jnp.concatenate([db[c, x, j] for c, x in places], axis=0)
        dn[j] = right3(inverse, 0)
        dt[j] = right3(inverse, 1)
    fy.end()

    fy.done()

    def block(l, j):
        cols = pl.ds(lane_of(l) + KP * j, KP)
        return jnp.concatenate([fb[c, x, :, :, cols].reshape(32, KP) for c, x in places], axis=0)

    for s in range(PANELS):
        cols = pl.ds(KP * s, KP)
        held = [qb[:, :, y, :, cols].reshape(64, KP) for y in range(4)]
        for k in range(4):
            rows = jnp.concatenate([held[y][:, 64 * k : 64 * k + 64] for y in range(4)], axis=1)
            for c in range(2):
                for x in range(CHIPS):
                    n = 8 * (4 * c + x)
                    qs[2 * x + c, k] = rows[n : n + 8]
        qt[:, pl.ds(KP * s, KP)] = jnp.transpose(qs[...].reshape(KP, KP))
    mine = pl.ds(pl.multiple_of(32 * own, 32), 32)
    for j in range(PANELS):
        y = qt[mine, pl.ds(KP * j, KP)]
        for l in range(j):
            y = y - dot_nt(xv[:, pl.ds(KP * l, KP)], block(j, l))
        xv[:, pl.ds(KP * j, KP)] = jnp.dot(left3(y, 1), dn[j], preferred_element_type=F32)
    for s in upward:
        r_ring[s].end()
    for j in range(PANELS):
        cols = pl.ds(KP * j, KP)
        f = fa[:, :, cols]
        m_of = lax.broadcasted_iota(jnp.int32, f.shape, 0)
        f = jnp.where(m_of * RING + q.z > j, f, 0.0)
        av[pl.ds(0, 128), cols] = f.reshape(128, KP)
        av[pl.ds(128, 32), cols] = xv[:, cols]
    for j in reversed(range(PANELS)):
        cols = pl.ds(KP * j, KP)
        y = av[:, cols]
        for l in range(j + 1, PANELS):
            y = y - dot_nn(gout[:, pl.ds(KP * l, KP)], block(l, j))
        gout[:, cols] = lax.dot_general(
            left3(y, 1), dt[j], (((1,), (1,)), ((), ())), preferred_element_type=F32
        )

    tq = jnp.zeros((128, 64), F32)
    yrows = pl.ds(pl.multiple_of(64 * q.y, 64), 64)
    for s in range(PANELS):
        cols = pl.ds(KP * s, KP)
        tq = tq + dot_nt(gout[pl.ds(0, 128), cols], qt[yrows, cols])
    tq_ref[...] = ql[...].reshape(128, 64) - tq

    for n, s in enumerate((3, 2, 1, 0)):
        r_ring[s].done()
        part = dot_nt(gout[:, pl.ds(KP * s, KP)], rbuf[s].reshape(512, KP))
        acc[...] = part if n == 0 else acc[...] + part
    slab = main.third()
    trail_ref[...] = jnp.transpose(slab) - acc[pl.ds(0, 128), :]
    scores_ref[...] = acc[pl.ds(128, 32), :] * (1.0 / math.sqrt(KP * PANELS))

    for s in range(PANELS):
        for k in range(4):
            for way in range(2):
                @pl.when(goes(s, way))
                def _(s=s, k=k, way=way):
                    chain(s, k, way).wait_send()
        r_ring[s].drain()

        for way in range(2):
            @pl.when(goes(s, way))
            def _(s=s, way=way):
                for part in parts_of(s):
                    row_copy(s, way, part).wait_send()
    for ring in (fx, fy, dx, dy):
        ring.drain()
    main.drain()
    pl.when(source)(panel.drain)


def finish(scores_in, trail_in, tq_in, scores_ref, trail_ref, tq_ref):
    scores_ref[...] = scores_in[...]
    trail_ref[...] = trail_in[...]
    tq_ref[...] = tq_in[...]


def per_device(gradients, projection, factor, diag_inverse, queries):
    vm = lambda *shape: pltpu.VMEM(shape, F32)
    dma = pltpu.SemaphoreType.DMA
    any_space = pl.BlockSpec(memory_space=pl.ANY)
    vmem_space = pl.BlockSpec(memory_space=pltpu.VMEM)
    shapes = (
        jax.ShapeDtypeStruct((32, 512), F32),
        jax.ShapeDtypeStruct((128, 512), F32),
        jax.ShapeDtypeStruct((128, 64), F32),
    )
    results = pl.pallas_call(
        kernel,
        out_shape=shapes,
        in_specs=[any_space] * 5,
        out_specs=(vmem_space,) * 3,
        scratch_shapes=[
            vm(512, 1024), vm(8192, 128),
            pltpu.VMEM((512, 3072), BF16), pltpu.VMEM((3072, 256), BF16),
            vm(4, 32, 1024), vm(4, 32, 64),
            vm(4, 8, 64, 256), vm(8, 512, 128),
            vm(4, 64, 256), vm(2, 32, 256), vm(2, 64, 256),
            vm(4, 512, 128), vm(2, 256, 128), vm(2, 512, 128),
            vm(4, 8, 64, 256), vm(2, 4, 4, 32, 256), vm(2, 4, 4, 8, 1536), vm(2, 4, 4, 8, 1024),
            vm(8, 4, 8, 256), vm(256, 1024), vm(32, 1024), vm(160, 1024), vm(160, 1024), vm(160, 512),
            pltpu.VMEM((4, 768, 256), BF16), pltpu.VMEM((4, 256, 768), BF16),
            dma((6,)), dma((10,)), dma((10,)), dma((10,)), dma((10,)),
            dma((10, 8)), dma((10, 8)), dma((4, 4, 2)), dma((4, 4)), dma((4, 2, 2)), dma((4, 2)),
        ],
        compiler_params=pltpu.CompilerParams(
            collective_id=0, has_side_effects=True, vmem_limit_bytes=60 * 1024 * 1024
        ),
    )(
        gradients,
        projection.reshape(8192, 128),
        factor.reshape(4, 32, 1024),
        diag_inverse,
        queries.reshape(4, 32, 64),
    )
    scores, trailing, trailing_queries = pl.pallas_call(
        finish, out_shape=shapes, in_specs=[vmem_space] * 3, out_specs=(vmem_space,) * 3
    )(*results)
    return (
        scores,
        trailing.reshape(4, 1, 32, 512),
        trailing_queries.reshape(4, 1, 32, 64),
    )


def solution(mesh):
    return jax.shard_map(
        per_device,
        mesh=mesh,
        in_specs=(
            P("ex", "param"),
            P("param", None, "feat", None),
            P(None, "feat", "param", None),
            P(None, "param", None),
            P(None, "feat", "param", "ex"),
        ),
        out_specs=(
            P("param", "ex"),
            P(None, "feat", "param", "ex"),
            P(None, "feat", "param", "ex"),
        ),
        check_vma=False,
    )
```

```python
import math

import jax
import jax.numpy as jnp
from jax import lax
from jax.experimental import pallas as pl
from jax.experimental.pallas import tpu as pltpu
from jax.sharding import PartitionSpec as P

MESH = pl.DeviceIdType.MESH
F32 = jnp.float32
BF16 = jnp.bfloat16
CHIPS = 4
PANELS = 4
RING = 16
UP = 8
KP = 256


def halves(x):
    hi = x.astype(BF16)
    return hi, (x - hi.astype(F32)).astype(BF16)


def left3(x, axis):
    hi, lo = halves(x)
    return jnp.concatenate([hi, lo, hi], axis=axis)


def right3(x, axis):
    hi, lo = halves(x)
    return jnp.concatenate([hi, hi, lo], axis=axis)


def dot_nn(a, b):
    return jnp.dot(left3(a, 1), right3(b, 0), preferred_element_type=F32)


def dot_nt(a, b):
    return lax.dot_general(
        left3(a, 1), right3(b, 1), (((1,), (1,)), ((), ())), preferred_element_type=F32
    )


class Place:
    def __init__(self):
        self.p = lax.axis_index("param")
        self.z = lax.axis_index("feat")
        self.y = lax.axis_index("ex")
        self.x = lax.div(self.p, 2)
        self.c = lax.rem(self.p, 2)
        self.xp = lax.rem(self.x + 1, CHIPS)
        self.xm = lax.rem(self.x + CHIPS - 1, CHIPS)
        self.xo = lax.rem(self.x + 2, CHIPS)
        self.right = {"param": 2 * self.xp + self.c}
        self.left = {"param": 2 * self.xm + self.c}
        self.sib = {"param": 2 * self.x + 1 - self.c}
        self.front = {"ex": lax.rem(self.y + 1, 4)}
        self.back = {"ex": lax.rem(self.y + 3, 4)}
        self.above = {"feat": lax.rem(self.z + 1, RING)}
        self.below = {"feat": lax.rem(self.z + RING - 1, RING)}

    def slot(self, x, c):
        return 2 * x + c


def rdma(src, dst, ss, rs, dev):
    return pltpu.make_async_remote_copy(
        src_ref=src, dst_ref=dst, send_sem=ss, recv_sem=rs, device_id=dev, device_id_type=MESH
    )


class Ring:
    def __init__(self, me, ahead, behind, sib, chunk, half_a, half_b, other, ss, rs):
        self.me, self.m, self.p, self.o = me, lax.rem(me + 3, 4), lax.rem(me + 1, 4), lax.rem(me + 2, 4)
        self.ahead, self.behind, self.sib = ahead, behind, sib
        self.chunk, self.half_a, self.half_b, self.other = chunk, half_a, half_b, other
        self.ss, self.rs = ss, rs

    def copy(self, k):
        ref, dev = (
            lambda: (self.chunk(self.me), self.ahead),
            lambda: (self.chunk(self.me), self.behind),
            lambda: (self.half_a(self.m), self.ahead),
            lambda: (self.half_b(self.p), self.behind),
            lambda: (self.chunk(self.me), self.sib),
            lambda: (self.chunk(self.m), self.sib),
            lambda: (self.chunk(self.p), self.sib),
            lambda: (self.chunk(self.o), self.sib),
        )[k]()
        return rdma(ref, ref, self.ss.at[k], self.rs.at[k], dev)

    def send(self, k):
        if k < 4 or self.other is not None:
            self.copy(k).start()

    def arrive(self, ref, k):
        rdma(ref, ref, self.ss.at[k], self.rs.at[k], self.sib).wait_recv()

    def start(self):
        for k in (0, 1, 4):
            self.send(k)

    def mid(self):
        self.arrive(self.chunk(self.m), 0)
        self.send(2)
        self.send(5)
        self.arrive(self.chunk(self.p), 1)
        self.send(3)
        self.send(6)

    def end(self):
        self.arrive(self.half_a(self.o), 2)
        self.arrive(self.half_b(self.o), 3)
        self.send(7)

    def done(self):
        for k, n in ((4, self.me), (5, self.m), (6, self.p), (7, self.o)):
            self.arrive(self.other(n), k)

    def drain(self):
        for k in range(4 if self.other is None else 8):
            self.copy(k).wait_send()


class Both:
    def __init__(self, *rings):
        self.rings = rings

    def __getattr__(self, name):
        def step():
            for ring in self.rings:
                getattr(ring, name)()

        return step


class Reduce:
    def __init__(self, pos, parts, got, relay, direct, rows, ss, rs):
        self.pos, self.parts, self.got, self.relay, self.direct = pos, parts, got, relay, direct
        self.h, self.ss, self.rs = rows // 2, ss, rs
        self.a, self.b = pl.ds(0, self.h), pl.ds(self.h, self.h)

    def pair_copy(self, x):
        q = self.pos
        return rdma(self.parts(q.slot(x, 1 - q.c)), self.got.at[x], self.ss.at[x], self.rs.at[x], q.sib)

    def x_copy(self, k):
        q, g = self.pos, self.got
        src, dst, dev = (
            lambda: (g.at[q.xo, self.a], self.relay.at[0], q.right),
            lambda: (g.at[q.xo, self.b], self.relay.at[1], q.left),
            lambda: (g.at[q.xp, self.b], self.direct.at[0, self.b], q.right),
            lambda: (g.at[q.xm, self.a], self.direct.at[1, self.a], q.left),
            lambda: (g.at[q.xp, self.a], self.direct.at[0, self.a], q.right),
            lambda: (g.at[q.xm, self.b], self.direct.at[1, self.b], q.left),
        )[k]()
        return rdma(src, dst, self.ss.at[4 + k], self.rs.at[4 + k], dev)

    def pair(self):
        for x in range(CHIPS):
            self.pair_copy(x).start()

    def first(self):
        q, g = self.pos, self.got
        for x in range(CHIPS):
            self.pair_copy(x).wait_recv()
        for n, x in enumerate((q.xo, q.xp, q.xm, q.x)):
            g[x] = g[x] + self.parts(q.slot(x, q.c))[...]
            if n == 0:
                self.x_copy(0).start()
                self.x_copy(1).start()
            elif n < 3:
                self.x_copy(n + 1).start()

    def second(self):
        q, g = self.pos, self.got
        self.x_copy(0).wait_recv()
        g[q.xp, self.a] = g[q.xp, self.a] + self.relay[0]
        self.x_copy(4).start()
        self.x_copy(1).wait_recv()
        g[q.xm, self.b] = g[q.xm, self.b] + self.relay[1]
        self.x_copy(5).start()

    def third(self):
        for k in range(2, 6):
            self.x_copy(k).wait_recv()
        return self.got[self.pos.x] + self.direct[0] + self.direct[1]

    def drain(self):
        for x in range(CHIPS):
            self.pair_copy(x).wait_send()
        for k in range(6):
            self.x_copy(k).wait_send()


def kernel(
    g_hbm, p_hbm, f_hbm, d_hbm, q_hbm, scores_ref, trail_ref, tq_ref,
    gv, pv, g3, p3, fa, ql, parts, slabs,
    pan_got, pan_relay, pan_direct, got, relay, direct,
    rbuf, db, fb, qb, qs, qt, xv, av, gout, acc,
    dn, dt, loc, ps, pr, ms, mr, gs, gr, zs, zr, fs, fr,
):
    q = Place()
    own = q.slot(q.x, q.c)
    source = q.z < PANELS

    def lane_of(s):
        return 128 * s * (s - 1)

    def load(k):
        return (
            lambda: pltpu.make_async_copy(g_hbm, gv, loc.at[0]),
            lambda: pltpu.make_async_copy(p_hbm, pv, loc.at[1]),
            lambda: pltpu.make_async_copy(d_hbm.at[q.y], db.at[q.c, q.x, q.y], loc.at[2]),
            lambda: pltpu.make_async_copy(q_hbm, ql, loc.at[3]),
            lambda: pltpu.make_async_copy(f_hbm, fa, loc.at[4]),
        )[k]()

    for k in range(5):
        load(k).start()

    def rows_of(s):
        return pltpu.make_async_copy(
            f_hbm.at[0, pl.ds(pl.multiple_of(8 * q.y, 8), 8), pl.ds(0, KP * s)],
            fb.at[q.c, q.x, q.y, :, pl.ds(lane_of(s), KP * s)],
            loc.at[5],
        )

    for s in range(1, PANELS):
        @pl.when(q.z == s)
        def _(s=s):
            rows_of(s).start()

    barrier = pltpu.get_barrier_semaphore()

    def greet(dev):
        pl.semaphore_signal(barrier, inc=1, device_id=dev, device_id_type=MESH)

    for dev in [q.right, q.left, q.sib, q.front, q.back, q.above, q.below]:
        greet(dev)
    low, high = pl.ds(0, 2), pl.ds(2, 2)
    r_ring = [
        Ring(
            q.x, q.right, q.left, q.sib,
            lambda n, s=s: rbuf.at[s, q.slot(n, q.c)],
            lambda n, s=s: rbuf.at[s, q.slot(n, q.c), pl.ds(0, 32)],
            lambda n, s=s: rbuf.at[s, q.slot(n, q.c), pl.ds(32, 32)],
            lambda n, s=s: rbuf.at[s, q.slot(n, 1 - q.c)],
            gs.at[s], gr.at[s],
        )
        for s in range(PANELS)
    ]
    fx = Both(
        Ring(
            q.x, q.right, q.left, q.sib,
            lambda n: fb.at[q.c, n, q.y],
            lambda n: fb.at[q.c, n, q.y, :, pl.ds(0, 768)],
            lambda n: fb.at[q.c, n, q.y, :, pl.ds(768, 768)],
            None, gs.at[4], gr.at[4],
        ),
        Ring(
            q.y, q.front, q.back, q.sib,
            lambda n: qb.at[q.c, q.x, n],
            lambda n: qb.at[q.c, q.x, n, :, pl.ds(0, 512)],
            lambda n: qb.at[q.c, q.x, n, :, pl.ds(512, 512)],
            None, gs.at[8], gr.at[8],
        ),
    )
    fy = Both(
        Ring(
            q.y, q.front, q.back, q.sib,
            lambda n: fb.at[q.c, :, n],
            lambda n: fb.at[q.c, low, n],
            lambda n: fb.at[q.c, high, n],
            lambda n: fb.at[1 - q.c, :, n],
            gs.at[5], gr.at[5],
        ),
        Ring(
            q.x, q.right, q.left, q.sib,
            lambda n: qb.at[q.c, n],
            lambda n: qb.at[q.c, n, low],
            lambda n: qb.at[q.c, n, high],
            lambda n: qb.at[1 - q.c, n],
            gs.at[9], gr.at[9],
        ),
    )
    dx = Ring(
        q.x, q.right, q.left, q.sib,
        lambda n: db.at[q.c, n, q.y],
        lambda n: db.at[q.c, n, q.y, pl.ds(0, 16)],
        lambda n: db.at[q.c, n, q.y, pl.ds(16, 16)],
        None, gs.at[6], gr.at[6],
    )
    dy = Ring(
        q.y, q.front, q.back, q.sib,
        lambda n: db.at[q.c, :, n],
        lambda n: db.at[q.c, low, n],
        lambda n: db.at[q.c, high, n],
        lambda n: db.at[1 - q.c, :, n],
        gs.at[7], gr.at[7],
    )

    def hop_of(s):
        return lax.rem(q.z - s + RING, RING)

    def chain(s, k, way):
        ref = rbuf.at[s, own, pl.ds(16 * k, 16)]
        return rdma(ref, ref, zs.at[s, k, way], zr.at[s, k], (q.above, q.below)[way])

    def goes(s, way):
        hop = hop_of(s)
        return hop < UP if way == 0 else (hop == 0) | (hop > UP + 1)

    def chain_send(s, k):
        for way in range(2):
            @pl.when(goes(s, way))
            def _(way=way):
                chain(s, k, way).start()

    def pass_on(s):
        @pl.when(q.z != s)
        def _():
            for k in range(4):
                chain(s, k, 0).wait_recv()
                chain_send(s, k)

    def row_copy(s, way, part):
        if part == 0:
            ref = qb.at[q.c, q.x, q.y, :, pl.ds(KP * s, KP)]
        else:
            ref = fb.at[q.c, q.x, q.y, :, pl.ds(lane_of(s), KP * s)]
        return rdma(ref, ref, fs.at[s, way, part], fr.at[s, part], (q.above, q.below)[way])

    def parts_of(s):
        return range(1 if s == 0 else 2)

    def row_send(s):
        for way in range(2):
            @pl.when(goes(s, way))
            def _(way=way):
                for part in parts_of(s):
                    row_copy(s, way, part).start()

    def rows_hop(t):
        for s in range(PANELS):
            @pl.when((hop_of(s) == t) | ((hop_of(s) == RING - t) & (t < UP)))
            def _(s=s):
                for part in parts_of(s):
                    row_copy(s, 0, part).wait_recv()
                row_send(s)

    load(0).wait()
    for k in range(4):
        cols = pl.ds(k * 256, 256)
        hi, lo = halves(gv[:, cols])
        g3[:, cols] = hi
        g3[:, pl.ds(1024 + k * 256, 256)] = lo
        g3[:, pl.ds(2048 + k * 256, 256)] = hi
    load(3).wait()
    for s in range(PANELS):
        @pl.when(q.z == s)
        def _(s=s):
            mine = ql[0]
            qb[q.c, q.x, q.y, :, pl.ds(KP * s, KP)] = jnp.concatenate(
                [mine[8 * k : 8 * k + 8] for k in range(4)], axis=1
            )
            if s > 0:
                rows_of(s).wait()
    load(2).wait()
    pl.semaphore_wait(barrier, 7)
    for s in range(PANELS):
        @pl.when(q.z == s)
        def _(s=s):
            row_send(s)
    dx.start()
    load(1).wait()

    def project(m):
        for h in range(2):
            w = pv[pl.ds(2 * m + h, 1024, stride=8), :]
            hi, lo = halves(w)
            lanes = pl.ds(128 * h, 128)
            p3[pl.ds(0, 1024), lanes] = hi
            p3[pl.ds(1024, 1024), lanes] = hi
            p3[pl.ds(2048, 1024), lanes] = lo
        parts[m] = jnp.dot(g3[...], p3[...], preferred_element_type=F32).reshape(8, 64, 256)

    panel = Reduce(q, lambda i: parts.at[0, i], pan_got, pan_relay, pan_direct, 64, ps, pr)
    main = Reduce(q, lambda i: slabs.at[i], got, relay, direct, 512, ms, mr)

    down, upward = (0, 1, 2, 3), (3, 2, 1, 0)
    climbs = (q.z > 1) & (q.z < UP + 2)

    def sides(which):
        return (which & climbs, upward), (which & jnp.logical_not(climbs), down)

    project(0)
    pl.when(source)(panel.pair)
    project(1)
    pl.when(source)(panel.first)

    @pl.when(jnp.logical_not(source))
    def _():
        rows_hop(1)

    project(2)

    @pl.when(source)
    def _():
        rows_hop(1)
        panel.second()
        rows_hop(2)

    @pl.when(jnp.logical_not(source))
    def _():
        rows_hop(2)
        dx.mid()

    project(3)

    @pl.when(source)
    def _():
        rbuf[q.z, own] = panel.third()
        for s in range(PANELS):
            @pl.when(q.z == s)
            def _(s=s):
                for k in range(4):
                    chain_send(s, k)
        dx.mid()

    rows_hop(3)

    lane = lax.broadcasted_iota(jnp.int32, (512, 128), 1)
    for h in range(2):
        cols = pl.ds(128 * h, 128)
        rounds = [parts[m, :, :, cols].reshape(512, 128) for m in range(4)]
        for k in range(4):
            slab = None
            for m in range(4):
                turn = (32 * (m - k)) % 128
                moved = pltpu.roll(rounds[m], turn, 1) if turn else rounds[m]
                slab = moved if slab is None else jnp.where(lax.div(lane, 32) == m, moved, slab)
            slabs[4 * h + k] = slab
    main.pair()

    @pl.when(jnp.logical_not(source))
    def _():
        rows_hop(4)
        dx.end()
        dy.start()

    near = (q.z == PANELS) | (q.z == RING - 1)
    between = ((q.z > PANELS) & (q.z < PANELS + 3)) | ((q.z > RING - 4) & (q.z < RING - 1))
    late = (q.z == PANELS + 3) | (q.z == RING - 4)
    far = (q.z > PANELS + 3) & (q.z < RING - 4)

    def over_x(s):
        r_ring[s].start()

    for side, order in sides(source):
        @pl.when(side)
        def _(order=order):
            rows_hop(4)
            fx.start()
            pass_on(order[0])
            pass_on(order[1])
            main.first()
            dx.end()
            dy.start()
            pass_on(order[2])
            fx.mid()
            pass_on(order[3])
            dy.mid()
            fx.end()
            fy.start()
            for s in order:
                over_x(s)
            main.second()

    for side, order in sides(near):
        @pl.when(side)
        def _(order=order):
            fx.start()
            pass_on(order[0])
            main.first()
            pass_on(order[1])
            fx.mid()
            pass_on(order[2])
            dy.mid()
            fx.end()
            fy.start()
            for s in order[:3]:
                over_x(s)
            pass_on(order[3])
            over_x(order[3])
            main.second()

    for side, order in sides(between):
        @pl.when(side)
        def _(order=order):
            main.first()
            rows_hop(5)
            rows_hop(6)
            dy.mid()
            fx.start()
            pass_on(order[0])
            main.second()
            fx.mid()
            pass_on(order[1])
            fx.end()
            fy.start()
            for s in order[:2]:
                over_x(s)
            pass_on(order[2])
            over_x(order[2])
            pass_on(order[3])
            over_x(order[3])

    for side, order in sides(late):
        @pl.when(side)
        def _(order=order):
            main.first()
            rows_hop(5)
            rows_hop(6)
            main.second()
            rows_hop(7)
            dy.mid()
            fx.start()
            pass_on(order[0])
            fx.mid()
            pass_on(order[1])
            fx.end()
            fy.start()
            for s in order[:2]:
                over_x(s)
            pass_on(order[2])
            over_x(order[2])
            pass_on(order[3])
            over_x(order[3])

    for side, order in sides(far):
        @pl.when(side)
        def _(order=order):
            main.first()
            rows_hop(5)
            rows_hop(6)
            main.second()
            rows_hop(7)
            rows_hop(8)
            dy.mid()
            fx.start()
            pass_on(order[0])
            fx.mid()
            pass_on(order[1])
            fx.end()
            fy.start()
            for s in order[:2]:
                over_x(s)
            pass_on(order[2])
            over_x(order[2])
            pass_on(order[3])
            over_x(order[3])

    for side, order in sides(q.z >= 0):
        @pl.when(side)
        def _(order=order):
            fy.mid()
            dy.end()
            for s in order:
                r_ring[s].mid()

    dy.done()
    load(4).wait()
    places = [(i % 2, i // 2) for i in range(8)]
    for j in range(PANELS):
        inverse = jnp.concatenate([db[c, x, j] for c, x in places], axis=0)
        dn[j] = right3(inverse, 0)
        dt[j] = right3(inverse, 1)
    fy.end()

    fy.done()

    def block(l, j):
        cols = pl.ds(lane_of(l) + KP * j, KP)
        return jnp.concatenate([fb[c, x, :, :, cols].reshape(32, KP) for c, x in places], axis=0)

    for s in range(PANELS):
        cols = pl.ds(KP * s, KP)
        held = [qb[:, :, y, :, cols].reshape(64, KP) for y in range(4)]
        for k in range(4):
            rows = jnp.concatenate([held[y][:, 64 * k : 64 * k + 64] for y in range(4)], axis=1)
            for c in range(2):
                for x in range(CHIPS):
                    n = 8 * (4 * c + x)
                    qs[2 * x + c, k] = rows[n : n + 8]
        qt[:, pl.ds(KP * s, KP)] = jnp.transpose(qs[...].reshape(KP, KP))
    mine = pl.ds(pl.multiple_of(32 * own, 32), 32)
    for j in range(PANELS):
        y = qt[mine, pl.ds(KP * j, KP)]
        for l in range(j):
            y = y - dot_nt(xv[:, pl.ds(KP * l, KP)], block(j, l))
        xv[:, pl.ds(KP * j, KP)] = jnp.dot(left3(y, 1), dn[j], preferred_element_type=F32)
    for s in upward:
        r_ring[s].end()
    for j in range(PANELS):
        cols = pl.ds(KP * j, KP)
        f = fa[:, :, cols]
        m_of = lax.broadcasted_iota(jnp.int32, f.shape, 0)
        f = jnp.where(m_of * RING + q.z > j, f, 0.0)
        av[pl.ds(0, 128), cols] = f.reshape(128, KP)
        av[pl.ds(128, 32), cols] = xv[:, cols]
    for j in reversed(range(PANELS)):
        cols = pl.ds(KP * j, KP)
        y = av[:, cols]
        for l in range(j + 1, PANELS):
            y = y - dot_nn(gout[:, pl.ds(KP * l, KP)], block(l, j))
        gout[:, cols] = lax.dot_general(
            left3(y, 1), dt[j], (((1,), (1,)), ((), ())), preferred_element_type=F32
        )

    tq = jnp.zeros((128, 64), F32)
    yrows = pl.ds(pl.multiple_of(64 * q.y, 64), 64)
    for s in range(PANELS):
        cols = pl.ds(KP * s, KP)
        tq = tq + dot_nt(gout[pl.ds(0, 128), cols], qt[yrows, cols])
    tq_ref[...] = ql[...].reshape(128, 64) - tq

    for n, s in enumerate((3, 2, 1, 0)):
        r_ring[s].done()
        part = dot_nt(gout[:, pl.ds(KP * s, KP)], rbuf[s].reshape(512, KP))
        acc[...] = part if n == 0 else acc[...] + part
    slab = main.third()
    trail_ref[...] = jnp.transpose(slab) - acc[pl.ds(0, 128), :]
    scores_ref[...] = acc[pl.ds(128, 32), :] * (1.0 / math.sqrt(KP * PANELS))

    for s in range(PANELS):
        for k in range(4):
            for way in range(2):
                @pl.when(goes(s, way))
                def _(s=s, k=k, way=way):
                    chain(s, k, way).wait_send()
        r_ring[s].drain()

        for way in range(2):
            @pl.when(goes(s, way))
            def _(s=s, way=way):
                for part in parts_of(s):
                    row_copy(s, way, part).wait_send()
    for ring in (fx, fy, dx, dy):
        ring.drain()
    main.drain()
    pl.when(source)(panel.drain)


def finish(scores_in, trail_in, tq_in, scores_ref, trail_ref, tq_ref):
    scores_ref[...] = scores_in[...]
    trail_ref[...] = trail_in[...]
    tq_ref[...] = tq_in[...]


def per_device(gradients, projection, factor, diag_inverse, queries):
    vm = lambda *shape: pltpu.VMEM(shape, F32)
    dma = pltpu.SemaphoreType.DMA
    any_space = pl.BlockSpec(memory_space=pl.ANY)
    vmem_space = pl.BlockSpec(memory_space=pltpu.VMEM)
    shapes = (
        jax.ShapeDtypeStruct((32, 512), F32),
        jax.ShapeDtypeStruct((128, 512), F32),
        jax.ShapeDtypeStruct((128, 64), F32),
    )
    results = pl.pallas_call(
        kernel,
        out_shape=shapes,
        in_specs=[any_space] * 5,
        out_specs=(vmem_space,) * 3,
        scratch_shapes=[
            vm(512, 1024), vm(8192, 128),
            pltpu.VMEM((512, 3072), BF16), pltpu.VMEM((3072, 256), BF16),
            vm(4, 32, 1024), vm(4, 32, 64),
            vm(4, 8, 64, 256), vm(8, 512, 128),
            vm(4, 64, 256), vm(2, 32, 256), vm(2, 64, 256),
            vm(4, 512, 128), vm(2, 256, 128), vm(2, 512, 128),
            vm(4, 8, 64, 256), vm(2, 4, 4, 32, 256), vm(2, 4, 4, 8, 1536), vm(2, 4, 4, 8, 1024),
            vm(8, 4, 8, 256), vm(256, 1024), vm(32, 1024), vm(160, 1024), vm(160, 1024), vm(160, 512),
            pltpu.VMEM((4, 768, 256), BF16), pltpu.VMEM((4, 256, 768), BF16),
            dma((6,)), dma((10,)), dma((10,)), dma((10,)), dma((10,)),
            dma((10, 8)), dma((10, 8)), dma((4, 4, 2)), dma((4, 4)), dma((4, 2, 2)), dma((4, 2)),
        ],
        compiler_params=pltpu.CompilerParams(
            collective_id=0, has_side_effects=True, vmem_limit_bytes=60 * 1024 * 1024
        ),
    )(
        gradients,
        projection.reshape(8192, 128),
        factor.reshape(4, 32, 1024),
        diag_inverse,
        queries.reshape(4, 32, 64),
    )
    scores, trailing, trailing_queries = pl.pallas_call(
        finish, out_shape=shapes, in_specs=[vmem_space] * 3, out_specs=(vmem_space,) * 3
    )(*results)
    return (
        scores,
        trailing.reshape(4, 1, 32, 512),
        trailing_queries.reshape(4, 1, 32, 64),
    )


def solution(mesh):
    return jax.shard_map(
        per_device,
        mesh=mesh,
        in_specs=(
            P("ex", "param"),
            P("param", None, "feat", None),
            P(None, "feat", "param", None),
            P(None, "param", None),
            P(None, "feat", "param", "ex"),
        ),
        out_specs=(
            P("param", "ex"),
            P(None, "feat", "param", "ex"),
            P(None, "feat", "param", "ex"),
        ),
        check_vma=False,
    )
```
